8 devices in a mesh: dp: 1 (over z), tp: 2 (over y), ep: 4 (over x, core).
Axes of the slice: x: 2, y: 2, z: 1, core: 2. Of those that a mesh axis runs over, the one named last changes fastest.
Arguments:
- hidden: bfloat16 [2048, 1024], P(('dp', 'ep'))
- seq_lens: int32 [2048], P(('dp', 'ep'))
- rope_cos: float32 [2048, 32], P(('dp', 'ep'))
- rope_sin: float32 [2048, 32], P(('dp', 'ep'))
- ln1_scale: bfloat16 [1024], replicated
- ln1_bias: bfloat16 [1024], replicated
- w_qkv: bfloat16 [1024, 2048], P(None, 'tp')
- b_qkv: bfloat16 [2048], P('tp')
- w_out: bfloat16 [1024, 1024], P('tp')
- b_out: bfloat16 [1024], replicated
- k_cache: bfloat16 [2048, 128, 8, 64], P(('dp', 'ep'), None, 'tp')
- v_cache: bfloat16 [2048, 128, 8, 64], P(('dp', 'ep'), None, 'tp')
- ln2_scale: bfloat16 [1024], replicated
- ln2_bias: bfloat16 [1024], replicated
- w_router: bfloat16 [1024, 32], replicated
- expert_ids: int32 [2048, 8], P(('dp', 'ep'))
- w_gate: bfloat16 [32, 1024, 512], P('ep', None, 'tp')
- w_up: bfloat16 [32, 1024, 512], P('ep', None, 'tp')
- w_down: bfloat16 [32, 512, 1024], P('ep', 'tp')
Outputs:
- output 1: bfloat16 [2048, 1024], P(('dp', 'ep'))
- output 2: bfloat16 [2048, 128, 8, 64], P(('dp', 'ep'), None, 'tp')
- output 3: bfloat16 [2048, 128, 8, 64], P(('dp', 'ep'), None, 'tp')
All inputs are finite; a program needn't handle non-finite values.
Results may differ from the reference program's by a relative error of at most 0.0106167.
Values are sent between devices in bfloat16 or wider.
A program may use at most 1 GiB of HBM per device.

```python
import jax
import jax.numpy as jnp
from jax import lax

D = 1024
HEADS = 16
KV_HEADS = 8
HEAD = 64
EXPERTS = 32
TOP = 8
FF = 512
BATCH = 512
SMAX = 128
EP_SHARDS = 4

TOKENS = EP_SHARDS * BATCH
Q_PER_GROUP = HEADS // KV_HEADS
QKV_COLS = KV_HEADS * (Q_PER_GROUP + 2) * HEAD
CAP = (2 * TOP * BATCH + EXPERTS - 1) // EXPERTS
EPS = 1e-5
ROPE_BASE = 10000.0


def gaussian(one_key, out_shape):
    return jax.random.normal(one_key, out_shape, jnp.float32)


def draw_routing(route_key):
    hot_key, shard_key = jax.random.split(route_key)
    hot_order = jax.random.permutation(hot_key, EXPERTS)
    n_pairs = TOP * BATCH
    even_total = n_pairs - n_pairs // 2
    even_rows = even_total // EXPERTS + (jnp.arange(EXPERTS) < even_total % EXPERTS).astype(jnp.int32)

    def one_shard(one_key):
        even_key, order_key = jax.random.split(one_key)
        even_order = jax.random.permutation(even_key, EXPERTS)
        counts = jnp.zeros((EXPERTS,), jnp.int32).at[even_order].set(even_rows)
        free_room = CAP - counts[hot_order]
        before = jnp.cumsum(free_room) - free_room
        extra_rows = jnp.minimum(jnp.maximum(n_pairs // 2 - before, 0), free_room)
        counts = counts.at[hot_order].add(extra_rows)
        run_ends = jnp.cumsum(counts)
        slot_expert = jnp.sum((jnp.arange(n_pairs)[:, None] >= run_ends[None, :]).astype(jnp.int32), axis=1)
        choices = slot_expert.reshape(TOP, BATCH).T
        return choices[jax.random.permutation(order_key, BATCH)]

    picked = jax.vmap(one_shard)(jax.random.split(shard_key, EP_SHARDS))
    return picked.reshape(TOKENS, TOP).astype(jnp.int32)


def draw_lengths(len_key):
    draw_key, mark_key = jax.random.split(len_key)
    lengths = jax.random.randint(draw_key, (TOKENS,), SMAX // 16, SMAX)
    mark_order = jax.random.permutation(mark_key, TOKENS)
    lengths = lengths.at[mark_order[0]].set(SMAX - 1).at[mark_order[1]].set(SMAX // 16)
    return lengths.astype(jnp.int32)


def draw_rope(rope_key, lengths, factor_min, factor_max):
    rescale = jax.random.uniform(rope_key, (HEAD // 2,), jnp.float32, factor_min, factor_max)
    inv_freq = ROPE_BASE ** (-jnp.arange(HEAD // 2, dtype=jnp.float32) * 2.0 / HEAD)
    angles = lengths.astype(jnp.float32)[:, None] * inv_freq[None, :] / rescale[None, :]
    return jnp.cos(angles), jnp.sin(angles)


def setup_inputs(seed: int = 0, part: int = 0) -> dict:
    shared_key = jax.random.key(seed)
    part_key = jax.random.fold_in(jax.random.key(seed + 1), part)
    weight_keys = jax.random.split(shared_key, 12)
    part_keys = jax.random.split(part_key, 7)
    bf16 = jnp.bfloat16
    lengths = draw_lengths(part_keys[0])
    rope_cos, rope_sin = draw_rope(part_keys[1], lengths, 1.0, 8.0)
    hidden = gaussian(part_keys[2], (TOKENS, D))
    k_cache = 2.0 * gaussian(part_keys[3], (TOKENS, SMAX, KV_HEADS, HEAD))
    v_cache = 0.5 * gaussian(part_keys[4], (TOKENS, 1, KV_HEADS, HEAD)) + gaussian(part_keys[5], (TOKENS, SMAX, KV_HEADS, HEAD))
    expert_ids = draw_routing(part_keys[6])
    return {
        'hidden': hidden.astype(bf16),
        'seq_lens': lengths,
        'rope_cos': rope_cos,
        'rope_sin': rope_sin,
        'ln1_scale': (1.0 + 0.3 * gaussian(weight_keys[0], (D,))).astype(bf16),
        'ln1_bias': (0.3 * gaussian(weight_keys[1], (D,))).astype(bf16),
        'w_qkv': (gaussian(weight_keys[2], (D, QKV_COLS)) * D ** -0.5).astype(bf16),
        'b_qkv': (0.5 * gaussian(weight_keys[3], (QKV_COLS,))).astype(bf16),
        'w_out': (gaussian(weight_keys[4], (HEADS * HEAD, D)) * (HEADS * HEAD) ** -0.5).astype(bf16),
        'b_out': (0.3 * gaussian(weight_keys[5], (D,))).astype(bf16),
        'k_cache': k_cache.astype(bf16),
        'v_cache': v_cache.astype(bf16),
        'ln2_scale': (1.0 + 0.3 * gaussian(weight_keys[6], (D,))).astype(bf16),
        'ln2_bias': (0.3 * gaussian(weight_keys[7], (D,))).astype(bf16),
        'w_router': (gaussian(weight_keys[8], (D, EXPERTS)) * D ** -0.5).astype(bf16),
        'expert_ids': expert_ids,
        'w_gate': (gaussian(weight_keys[9], (EXPERTS, D, FF)) * D ** -0.5).astype(bf16),
        'w_up': (gaussian(weight_keys[10], (EXPERTS, D, FF)) * D ** -0.5).astype(bf16),
        'w_down': (gaussian(weight_keys[11], (EXPERTS, FF, D)) * FF ** -0.5).astype(bf16),
    }


def layer_norm(values, ln_scale, ln_bias):
    vals_f32 = values.astype(jnp.float32)
    row_mean = jnp.mean(vals_f32, axis=-1, keepdims=True)
    centered = vals_f32 - row_mean
    row_var = jnp.mean(centered * centered, axis=-1, keepdims=True)
    normed = centered * lax.rsqrt(row_var + EPS)
    return (normed * ln_scale.astype(jnp.float32) + ln_bias.astype(jnp.float32)).astype(jnp.bfloat16)


def apply_rope(values, cos_part, sin_part):
    half_dim = values.shape[-1] // 2
    vals_f32 = values.astype(jnp.float32)
    first_half = vals_f32[..., :half_dim]
    second_half = vals_f32[..., half_dim:]
    rotated = jnp.concatenate([first_half * cos_part - second_half * sin_part, second_half * cos_part + first_half * sin_part], axis=-1)
    return rotated.astype(jnp.bfloat16)


def reference(hidden, seq_lens, rope_cos, rope_sin, ln1_scale, ln1_bias, w_qkv, b_qkv, w_out, b_out, k_cache, v_cache, ln2_scale, ln2_bias, w_router, expert_ids, w_gate, w_up, w_down):
    normed = layer_norm(hidden, ln1_scale, ln1_bias)
    qkv_rows = (jnp.dot(normed, w_qkv, preferred_element_type=jnp.float32) + b_qkv.astype(jnp.float32)).astype(jnp.bfloat16)
    qkv_rows = qkv_rows.reshape(TOKENS, KV_HEADS, Q_PER_GROUP + 2, HEAD)
    queries = apply_rope(qkv_rows[:, :, :Q_PER_GROUP], rope_cos[:, None, None, :], rope_sin[:, None, None, :])
    key_new = apply_rope(qkv_rows[:, :, Q_PER_GROUP], rope_cos[:, None, :], rope_sin[:, None, :])
    value_new = qkv_rows[:, :, Q_PER_GROUP + 1]
    positions = jnp.arange(SMAX)
    write_mask = (positions[None, :] == seq_lens[:, None])[:, :, None, None]
    k_cache_out = jnp.where(write_mask, key_new[:, None], k_cache)
    v_cache_out = jnp.where(write_mask, value_new[:, None], v_cache)

    def attend(per_seq):
        q_one, k_one, v_one, len_one = per_seq
        scores = jnp.einsum('gqh,sgh->gqs', q_one.astype(jnp.float32), k_one.astype(jnp.float32)) * HEAD ** -0.5
        scores = jnp.where(positions[None, None, :] <= len_one, scores, -jnp.inf)
        attn_probs = jax.nn.softmax(scores, axis=-1).astype(jnp.bfloat16)
        return jnp.einsum('gqs,sgh->gqh', attn_probs.astype(jnp.float32), v_one.astype(jnp.float32)).astype(jnp.bfloat16)

    context = lax.map(attend, (queries, k_cache_out, v_cache_out, seq_lens))
    attn_full = jnp.dot(context.reshape(TOKENS, HEADS * HEAD), w_out, preferred_element_type=jnp.float32)
    hidden_mid = (hidden.astype(jnp.float32) + attn_full + b_out.astype(jnp.float32)).astype(jnp.bfloat16)
    normed2 = layer_norm(hidden_mid, ln2_scale, ln2_bias)
    logits = jnp.dot(normed2, w_router, preferred_element_type=jnp.float32)
    chosen = jnp.take_along_axis(logits, expert_ids, axis=1)
    gate_probs = jax.nn.softmax(chosen, axis=-1).astype(jnp.bfloat16).astype(jnp.float32)
    mix_weights = jnp.sum(jax.nn.one_hot(expert_ids, EXPERTS, dtype=jnp.float32) * gate_probs[:, :, None], axis=1)

    def expert_step(moe_acc, per_expert):
        gate_w, up_w, down_w, weight = per_expert
        gate_pre = jnp.dot(normed2, gate_w, preferred_element_type=jnp.float32)
        up_pre = jnp.dot(normed2, up_w, preferred_element_type=jnp.float32)
        hidden_act = (jax.nn.silu(gate_pre) * up_pre).astype(jnp.bfloat16)
        expert_out = jnp.dot(hidden_act, down_w, preferred_element_type=jnp.float32).astype(jnp.bfloat16)
        return moe_acc + weight[:, None] * expert_out.astype(jnp.float32), None

    moe_sum, _ = lax.scan(expert_step, jnp.zeros((TOKENS, D), jnp.float32), (w_gate, w_up, w_down, mix_weights.T))
    hidden_out = (hidden_mid.astype(jnp.float32) + moe_sum).astype(jnp.bfloat16)
    return (hidden_out, k_cache_out, v_cache_out)
```

```python
import functools

import jax
import jax.numpy as jnp
from jax import lax
from jax.experimental import pallas as pl
from jax.experimental.pallas import tpu as pltpu
from jax.sharding import PartitionSpec as P

EPS = 1e-5
BF = jnp.bfloat16
F32 = jnp.float32
CHUNKS = 1
SUB = 128
BB = 32
VMEM_LIMIT = 60 * 1024 * 1024


def norm_rows(x, scale, bias):
    mean = jnp.mean(x, axis=-1, keepdims=True)
    cen = x - mean
    var = jnp.mean(cen * cen, axis=-1, keepdims=True)
    return (cen * lax.rsqrt(var + EPS) * scale + bias).astype(BF)


def attention_kernel(len_ref, hid_ref, cos_ref, sin_ref, s1_ref, b1_ref, wqkv_ref, bqkv_ref, wout_ref, k_ref, v_ref, *rest):
    part_ref, ko_ref, vo_ref, qs_ref, kt_ref, vt_ref, sc_ref, pr_ref, cx_ref, ctx_ref = rest[-10:]
    i, j = pl.program_id(0), pl.program_id(1)
    n_j = pl.num_programs(1)
    lane = lax.broadcasted_iota(jnp.int32, (SUB, 128), 1)
    low = lane < 64

    @pl.when(j == 0)
    def _():
        normed = norm_rows(hid_ref[...].astype(F32), s1_ref[...].astype(F32), b1_ref[...].astype(F32))
        qkv = jnp.dot(normed, wqkv_ref[...], preferred_element_type=F32) + bqkv_ref[...].astype(F32)
        qkv = qkv.astype(BF).astype(F32)
        col = [qkv[:, m * 128:(m + 1) * 128] for m in range(8)]
        rol = [pltpu.roll(c, 64, 1) for c in col]

        def first(a, b):
            return jnp.where(low, col[a], rol[b])

        def second(a, b):
            return jnp.where(low, rol[a], col[b])

        cos_t, sin_t = cos_ref[...], sin_ref[...]
        cos = jnp.transpose(jnp.concatenate([cos_t] * 4, axis=0))
        sin = jnp.transpose(jnp.concatenate([-sin_t, sin_t] * 2, axis=0))

        def rope(x):
            other = jnp.where(lane % 64 < 32, pltpu.roll(x, 96, 1), pltpu.roll(x, 32, 1))
            return (x * cos + other * sin).astype(BF).astype(F32)

        for h in range(2):
            q0 = rope(first(4 * h, 4 * h + 2))
            q1 = rope(second(4 * h, 4 * h + 2))
            kk = rope(first(4 * h + 1, 4 * h + 3))
            vv = second(4 * h + 1, 4 * h + 3)
            kt_ref[h * 128:(h + 1) * 128, :] = jnp.transpose(kk)
            vt_ref[h * 128:(h + 1) * 128, :] = jnp.transpose(vv)
            for r in range(8):
                src = q0 if r % 2 == 0 else q1
                if r // 4 == h:
                    src = jnp.where(low if (r // 2) % 2 == 0 else ~low, src, 0.0)
                else:
                    src = jnp.zeros_like(src)
                qs_ref[pl.ds(h * SUB * 8 + r, SUB, stride=8), :] = src

    shift = lax.rem(SUB - j * BB, SUB)
    kt = pltpu.roll(kt_ref[...], shift, 1)
    vt = pltpu.roll(vt_ref[...], shift, 1)
    lane8 = lax.broadcasted_iota(jnp.int32, (8, 128), 1)
    lane256 = lax.broadcasted_iota(jnp.int32, (256, 128), 1)
    row0 = pl.multiple_of(j * BB * 8, BB * 8)
    base = i * SUB + j * BB
    for b in range(BB):
        pos = len_ref[base + b]
        hit = lane256 == pos
        k_old = k_ref[b].reshape(256, 128).astype(F32)
        k_new = jnp.where(hit, kt[:, b:b + 1], k_old).astype(BF)
        ko_ref[b] = k_new.reshape(4, 64, 128)
        q_one = jnp.concatenate([qs_ref[pl.ds(row0 + h * SUB * 8 + b * 8, 8), :] for h in range(2)], axis=1).astype(BF)
        s_one = jnp.dot(q_one, k_new, preferred_element_type=F32) * 0.125
        sc_ref[b * 8:(b + 1) * 8, :] = jnp.where(lane8 <= pos, s_one, -jnp.inf)
    s_all = sc_ref[...]
    e_all = jnp.exp(s_all - jnp.max(s_all, axis=-1, keepdims=True))
    pr_ref[...] = e_all / jnp.sum(e_all, axis=-1, keepdims=True)
    for b in range(BB):
        pos = len_ref[base + b]
        hit = lane256 == pos
        v_old = v_ref[b].reshape(256, 128).astype(F32)
        v_new = jnp.where(hit, vt[:, b:b + 1], v_old).astype(BF)
        vo_ref[b] = v_new.reshape(4, 64, 128)
        p_one = pr_ref[b * 8:(b + 1) * 8, :].astype(BF)
        c_one = lax.dot_general(p_one, v_new, (((1,), (1,)), ((), ())), preferred_element_type=F32)
        cx_ref[b * 8:(b + 1) * 8, :] = c_one[:, :128]
        cx_ref[BB * 8 + b * 8:BB * 8 + (b + 1) * 8, :] = c_one[:, 128:]
    low_b = lax.broadcasted_iota(jnp.int32, (BB, 128), 1) < 64
    for h in range(2):
        for g in range(2):
            r = 4 * h + 2 * g
            one = cx_ref[pl.ds(h * BB * 8 + r, BB, stride=8), :]
            two = cx_ref[pl.ds(h * BB * 8 + r + 1, BB, stride=8), :]
            if g == 0:
                both = jnp.where(low_b, one, pltpu.roll(two, 64, 1))
            else:
                both = jnp.where(low_b, pltpu.roll(one, 64, 1), two)
            ctx_ref[pl.ds(pl.multiple_of(j * BB, BB), BB), (2 * h + g) * 128:(2 * h + g + 1) * 128] = both.astype(BF)

    @pl.when(j == n_j - 1)
    def _():
        part_ref[...] = jnp.dot(ctx_ref[...], wout_ref[...], preferred_element_type=F32).astype(BF)


def attention(chunk, rows, lens, hidden, cos_t, sin_t, s1, b1, wqkv, bqkv, wout, kt, vt, prev):
    n_batch = hidden.shape[0]
    n_i, n_j = rows // SUB, SUB // BB
    first = chunk * n_i
    full = lambda shape: pl.BlockSpec(shape, lambda i, j, s: (0,) * len(shape), pipeline_mode=pl.Buffered(1))
    cache = pl.BlockSpec((BB, 4, 64, 128), lambda i, j, s: ((first + i) * n_j + j, 0, 0, 0))
    in_specs = [
        pl.BlockSpec((SUB, 1024), lambda i, j, s: (first + i, 0)),
        pl.BlockSpec((32, SUB), lambda i, j, s: (0, first + i)),
        pl.BlockSpec((32, SUB), lambda i, j, s: (0, first + i)),
        full((1, 1024)), full((1, 1024)), full((1024, 1024)), full((1, 1024)), full((512, 1024)),
        cache, cache,
    ]
    args = [lens[chunk * rows:(chunk + 1) * rows], hidden, cos_t, sin_t, s1, b1, wqkv, bqkv, wout, kt, vt]
    aliases = {}
    if prev is not None:
        in_specs += [pl.BlockSpec(memory_space=pl.ANY)] * 2
        aliases = {len(args): 1, len(args) + 1: 2}
        args += list(prev)
    return pl.pallas_call(
        attention_kernel,
        grid_spec=pltpu.PrefetchScalarGridSpec(
            num_scalar_prefetch=1, grid=(n_i, n_j), in_specs=in_specs,
            out_specs=[pl.BlockSpec((SUB, 1024), lambda i, j, s: (i, 0)), cache, cache],
            scratch_shapes=[
                pltpu.VMEM((2 * SUB * 8, 128), F32), pltpu.VMEM((256, SUB), F32), pltpu.VMEM((256, SUB), F32),
                pltpu.VMEM((BB * 8, 128), F32), pltpu.VMEM((BB * 8, 128), F32),
                pltpu.VMEM((2 * BB * 8, 128), F32), pltpu.VMEM((SUB, 512), BF)]),
        out_shape=[jax.ShapeDtypeStruct((rows, 1024), BF), jax.ShapeDtypeStruct(kt.shape, BF), jax.ShapeDtypeStruct(vt.shape, BF)],
        input_output_aliases=aliases,
        compiler_params=pltpu.CompilerParams(dimension_semantics=("arbitrary", "arbitrary"), vmem_limit_bytes=VMEM_LIMIT),
        cost_estimate=pl.CostEstimate(flops=rows * 20_000_000, bytes_accessed=rows * 262144, transcendentals=0),
        name="attention",
    )(*args)


def mid_kernel(hid_ref, one_ref, two_ref, bo_ref, s2_ref, b2_ref, x1_ref, h2_ref):
    attn = one_ref[...].astype(F32) + two_ref[...].astype(F32)
    x1 = (hid_ref[...].astype(F32) + attn + bo_ref[...].astype(F32)).astype(BF)
    x1_ref[...] = x1
    h2_ref[...] = norm_rows(x1.astype(F32), s2_ref[...].astype(F32), b2_ref[...].astype(F32))


def middle(chunk, rows, hidden, one, two, b_out, s2, b2):
    tile = 128
    off = chunk * rows // tile
    vec = pl.BlockSpec((1, 1024), lambda i: (0, 0))
    blk = pl.BlockSpec((tile, 1024), lambda i: (i, 0))
    return pl.pallas_call(
        mid_kernel, grid=(rows // tile,),
        in_specs=[pl.BlockSpec((tile, 1024), lambda i: (off + i, 0)), blk, blk, vec, vec, vec],
        out_specs=[blk, blk],
        out_shape=[jax.ShapeDtypeStruct((rows, 1024), BF)] * 2,
        cost_estimate=pl.CostEstimate(flops=rows * 400_000, bytes_accessed=rows * 10240, transcendentals=0),
        name="middle",
    )(hidden, one, two, b_out, s2, b2)


def expert_kernel(rows, first_ref, x0, x1, x2, x3, i0, i1, i2, i3, wr_ref, wg_ref, wu_ref, wd_ref, o0, o1, o2, o3, acc_ref, gate_ref):
    e = pl.program_id(0)
    n_e = pl.num_programs(0)
    xs, ids, outs = (x0, x1, x2, x3), (i0, i1, i2, i3), (o0, o1, o2, o3)
    tile = min(rows, 256)

    @pl.when(e == 0)
    def _():
        for n in range(4):
            logit = lax.dot_general(wr_ref[...], xs[n][...], (((1,), (1,)), ((), ())), preferred_element_type=F32)
            eid = lax.broadcasted_iota(jnp.int32, (32, rows), 0)
            picked = eid == ids[n][0:1, :]
            for m in range(1, 8):
                picked = picked | (eid == ids[n][m:m + 1, :])
            logit = jnp.where(picked, logit, -jnp.inf)
            ex = jnp.exp(logit - jnp.max(logit, axis=0, keepdims=True))
            prob = (ex / jnp.sum(ex, axis=0, keepdims=True)).astype(BF).astype(F32)
            gate_ref[n * rows:(n + 1) * rows, :] = jnp.transpose(prob)

    mine = first_ref[0] + e
    for n in range(4):
        for t in range(rows // tile):
            sl = slice(t * tile, (t + 1) * tile)
            row = n * rows + t * tile
            x = xs[n][sl, :]
            gate = jnp.dot(x, wg_ref[0], preferred_element_type=F32)
            up = jnp.dot(x, wu_ref[0], preferred_element_type=F32)
            act = (gate * jax.nn.sigmoid(gate) * up).astype(BF)
            y = jnp.dot(act, wd_ref[0], preferred_element_type=F32).astype(BF).astype(F32)
            g_all = gate_ref[row:row + tile, :]
            lane = lax.broadcasted_iota(jnp.int32, (tile, 32), 1)
            g_one = jnp.sum(jnp.where(lane == mine, g_all, 0.0), axis=-1, keepdims=True)
            term = g_one * y

            @pl.when(e == 0)
            def _():
                acc_ref[row:row + tile, :] = term

            @pl.when((e > 0) & (e < n_e - 1))
            def _():
                acc_ref[row:row + tile, :] += term

            @pl.when(e == n_e - 1)
            def _():
                outs[n][sl, :] = (acc_ref[row:row + tile, :] + term).astype(BF)


def experts(rows, first, xs, ids, wr_t, wg, wu, wd):
    n_e = wg.shape[0]
    full = lambda shape: pl.BlockSpec(shape, lambda e, s: (0,) * len(shape), pipeline_mode=pl.Buffered(1))
    wspec = lambda a: pl.BlockSpec((1,) + a.shape[1:], lambda e, s: (e, 0, 0))
    return pl.pallas_call(
        functools.partial(expert_kernel, rows),
        grid_spec=pltpu.PrefetchScalarGridSpec(
            num_scalar_prefetch=1, grid=(n_e,),
            in_specs=[full((rows, 1024))] * 4 + [full((8, rows))] * 4 + [full((32, 1024)), wspec(wg), wspec(wu), wspec(wd)],
            out_specs=[full((rows, 1024))] * 4,
            scratch_shapes=[pltpu.VMEM((4 * rows, 1024), F32), pltpu.VMEM((4 * rows, 32), F32)]),
        out_shape=[jax.ShapeDtypeStruct((rows, 1024), BF)] * 4,
        compiler_params=pltpu.CompilerParams(dimension_semantics=("arbitrary",), vmem_limit_bytes=VMEM_LIMIT),
        cost_estimate=pl.CostEstimate(flops=rows * 4 * n_e * 1_600_000, bytes_accessed=14_000_000, transcendentals=0),
        name="experts",
    )(first, *xs, *ids, wr_t, wg, wu, wd)


def solution(mesh):
    n_ep = mesh.shape['ep']
    token_rows = P(('dp', 'ep'), None)
    token_vec = P(('dp', 'ep'))
    cache_spec = P(('dp', 'ep'), None, 'tp', None)
    expert_in = P('ep', None, 'tp')
    expert_down = P('ep', 'tp', None)

    def swap_ep(x, bit):
        return lax.ppermute(x, 'ep', [(d, d ^ bit) for d in range(n_ep)])

    def swap_tp(x):
        return lax.ppermute(x, 'tp', [(0, 1), (1, 0)])

    def spread(x):
        far = swap_ep(x, 2)
        return [x, swap_ep(x, 1), far, swap_ep(far, 1)]

    def device_step(hidden, seq_lens, rope_cos, rope_sin, ln1_scale, ln1_bias, w_qkv, b_qkv, w_out, b_out, k_cache, v_cache, ln2_scale, ln2_bias, w_router, expert_ids, w_gate, w_up, w_down):
        n_batch = hidden.shape[0]
        rows = n_batch // CHUNKS
        kt, vt = (jnp.transpose(c, (0, 2, 3, 1)) for c in (k_cache, v_cache))
        row = lambda a: a.reshape(1, -1)
        ids = spread(expert_ids.T)
        first = (lax.axis_index('ep') * w_gate.shape[0]).astype(jnp.int32).reshape(1)
        prev = None
        outs = []
        for c in range(CHUNKS):
            part, *prev = attention(c, rows, seq_lens, hidden, rope_cos.T, rope_sin.T, row(ln1_scale), row(ln1_bias), w_qkv, row(b_qkv), w_out, kt, vt, prev)
            x1, h2 = middle(c, rows, hidden, part, swap_tp(part), row(b_out), row(ln2_scale), row(ln2_bias))
            cut = [a[:, c * rows:(c + 1) * rows] for a in ids]
            o = experts(rows, first, spread(h2), cut, w_router.T, w_gate, w_up, w_down)
            near = (o[0].astype(F32) + swap_ep(o[1], 1).astype(F32)).astype(BF)
            far = (o[2].astype(F32) + swap_ep(o[3], 1).astype(F32)).astype(BF)
            total = (near.astype(F32) + swap_ep(far, 2).astype(F32)).astype(BF)
            moe = total.astype(F32) + swap_tp(total).astype(F32)
            outs.append((x1.astype(F32) + moe).astype(BF))
        hidden_out = outs[0] if CHUNKS == 1 else jnp.concatenate(outs, axis=0)
        return hidden_out, *(jnp.transpose(c, (0, 3, 1, 2)) for c in prev)

    in_specs = (token_rows, token_vec, token_rows, token_rows, P(), P(), P(None, 'tp'), P('tp'), P('tp', None), P(), cache_spec, cache_spec, P(), P(), P(), token_rows, expert_in, expert_in, expert_down)
    return jax.shard_map(device_step, mesh=mesh, in_specs=in_specs, out_specs=(token_rows, cache_spec, cache_spec), check_vma=False)
```

```python
import functools

import jax
import jax.numpy as jnp
from jax import lax
from jax.experimental import pallas as pl
from jax.experimental.pallas import tpu as pltpu
from jax.sharding import PartitionSpec as P

EPS = 1e-5
BF = jnp.bfloat16
F32 = jnp.float32
CHUNKS = 4
SUB = 128
BB = 16
SLOTS = 8
AHEAD = 5
VMEM_LIMIT = 60 * 1024 * 1024


def norm_rows(x, scale, bias):
    mean = jnp.mean(x, axis=-1, keepdims=True)
    cen = x - mean
    var = jnp.mean(cen * cen, axis=-1, keepdims=True)
    return (cen * lax.rsqrt(var + EPS) * scale + bias).astype(BF)


def wide(ref):
    return ref[...].astype(F32).reshape(1, -1)


def attention_kernel(base_row, has_prev, len_ref, hid_ref, cos_ref, sin_ref, s1_ref, b1_ref, bqkv_ref, wqkv_hbm, wout_hbm, k_hbm, v_hbm, *rest):
    part_ref, ko_hbm, vo_hbm = rest[2 * has_prev:2 * has_prev + 3]
    wqkv_ref, wout_ref, kb_ref, vb_ref, qs_ref, kt_ref, vt_ref, sc_ref, pr_ref, cx_ref, ctx_ref, in_sem, out_sem, w_sem = rest[2 * has_prev + 3:]
    step = pl.program_id(0)
    n_step = pl.num_programs(0)
    per_sub = SUB // BB
    j = lax.rem(step, per_sub)
    lane = lax.broadcasted_iota(jnp.int32, (SUB, 128), 1)
    low = lane < 64

    def moves(s, out):
        slot = lax.rem(s, SLOTS)
        src = pl.ds(base_row + s * BB, BB)
        pairs = ((k_hbm, kb_ref, ko_hbm, 0), (v_hbm, vb_ref, vo_hbm, 1))
        if out:
            return [(pltpu.make_async_copy(buf.at[slot], dst.at[src], out_sem.at[t, slot]), t) for _, buf, dst, t in pairs]
        return [(pltpu.make_async_copy(hbm.at[src], buf.at[slot], in_sem.at[t, slot]), t) for hbm, buf, _, t in pairs]

    def begin(s, out):
        for copy, t in moves(s, out):
            copy.start(priority=t)

    def finish(s, out):
        for copy, _ in moves(s, out):
            copy.wait()

    load_qkv = pltpu.make_async_copy(wqkv_hbm, wqkv_ref, w_sem.at[0])
    load_out = pltpu.make_async_copy(wout_hbm, wout_ref, w_sem.at[1])

    @pl.when(step == 0)
    def _():
        load_qkv.start()
        for s in range(AHEAD):
            begin(s, False)
        load_out.start()
        load_qkv.wait()

    @pl.when(j == 0)
    def _():
        normed = norm_rows(hid_ref[...].astype(F32), wide(s1_ref), wide(b1_ref))
        qkv = jnp.dot(normed, wqkv_ref[...], preferred_element_type=F32) + wide(bqkv_ref)
        qkv = qkv.astype(BF).astype(F32)
        col = [qkv[:, m * 128:(m + 1) * 128] for m in range(8)]
        rol = [pltpu.roll(c, 64, 1) for c in col]

        def first(a, b):
            return jnp.where(low, col[a], rol[b])

        def second(a, b):
            return jnp.where(low, rol[a], col[b])

        cos_t, sin_t = cos_ref[...], sin_ref[...]
        cos = jnp.transpose(jnp.concatenate([cos_t] * 4, axis=0))
        sin = jnp.transpose(jnp.concatenate([-sin_t, sin_t] * 2, axis=0))

        def rope(x):
            other = jnp.where(lane % 64 < 32, pltpu.roll(x, 96, 1), pltpu.roll(x, 32, 1))
            return (x * cos + other * sin).astype(BF).astype(F32)

        for h in range(2):
            q0 = rope(first(4 * h, 4 * h + 2))
            q1 = rope(second(4 * h, 4 * h + 2))
            kk = rope(first(4 * h + 1, 4 * h + 3))
            vv = second(4 * h + 1, 4 * h + 3)
            kt_ref[h * 128:(h + 1) * 128, :] = jnp.transpose(kk)
            vt_ref[h * 128:(h + 1) * 128, :] = jnp.transpose(vv)
            for r in range(8):
                src = q0 if r % 2 == 0 else q1
                if r // 4 == h:
                    src = jnp.where(low if (r // 2) % 2 == 0 else ~low, src, 0.0)
                else:
                    src = jnp.zeros_like(src)
                qs_ref[pl.ds(h * SUB * 8 + r, SUB, stride=8), :] = src

    slot = lax.rem(step, SLOTS)
    finish(step, False)
    shift = lax.rem(SUB - j * BB, SUB)
    kt = pltpu.roll(kt_ref[...], shift, 1)
    vt = pltpu.roll(vt_ref[...], shift, 1)
    lane8 = lax.broadcasted_iota(jnp.int32, (8, 128), 1)
    lane256 = lax.broadcasted_iota(jnp.int32, (256, 128), 1)
    row0 = pl.multiple_of(j * BB * 8, BB * 8)
    base = base_row + step * BB
    for b in range(BB):
        pos = len_ref[base + b]
        k_old = kb_ref[slot, b].reshape(256, 128).astype(F32)
        k_new = jnp.where(lane256 == pos, kt[:, b:b + 1], k_old).astype(BF)
        kb_ref[slot, b] = k_new.reshape(4, 64, 128)
        q_one = jnp.concatenate([qs_ref[pl.ds(row0 + h * SUB * 8 + b * 8, 8), :] for h in range(2)], axis=1).astype(BF)
        s_one = jnp.dot(q_one, k_new, preferred_element_type=F32) * 0.125
        sc_ref[b * 8:(b + 1) * 8, :] = jnp.where(lane8 <= pos, s_one, -jnp.inf)
    s_all = sc_ref[...]
    e_all = jnp.exp(s_all - jnp.max(s_all, axis=-1, keepdims=True))
    pr_ref[...] = e_all / jnp.sum(e_all, axis=-1, keepdims=True)
    for b in range(BB):
        pos = len_ref[base + b]
        v_old = vb_ref[slot, b].reshape(256, 128).astype(F32)
        v_new = jnp.where(lane256 == pos, vt[:, b:b + 1], v_old).astype(BF)
        vb_ref[slot, b] = v_new.reshape(4, 64, 128)
        p_one = pr_ref[b * 8:(b + 1) * 8, :].astype(BF)
        c_one = lax.dot_general(p_one, v_new, (((1,), (1,)), ((), ())), preferred_element_type=F32)
        cx_ref[b * 8:(b + 1) * 8, :] = c_one[:, :128]
        cx_ref[BB * 8 + b * 8:BB * 8 + (b + 1) * 8, :] = c_one[:, 128:]
    low_b = lax.broadcasted_iota(jnp.int32, (BB, 128), 1) < 64
    for h in range(2):
        for g in range(2):
            r = 4 * h + 2 * g
            one = cx_ref[pl.ds(h * BB * 8 + r, BB, stride=8), :]
            two = cx_ref[pl.ds(h * BB * 8 + r + 1, BB, stride=8), :]
            if g == 0:
                both = jnp.where(low_b, one, pltpu.roll(two, 64, 1))
            else:
                both = jnp.where(low_b, pltpu.roll(one, 64, 1), two)
            ctx_ref[pl.ds(pl.multiple_of(j * BB, BB), BB), (2 * h + g) * 128:(2 * h + g + 1) * 128] = both.astype(BF)

    begin(step, True)

    @pl.when(step + AHEAD < n_step)
    def _():
        @pl.when(step + AHEAD >= SLOTS)
        def _():
            finish(step + AHEAD - SLOTS, True)

        begin(step + AHEAD, False)

    @pl.when(step == per_sub - 1)
    def _():
        load_out.wait()

    @pl.when(j == per_sub - 1)
    def _():
        part_ref[...] = jnp.dot(ctx_ref[...], wout_ref[...], preferred_element_type=F32).astype(BF)

    @pl.when(step == n_step - 1)
    def _():
        for back in range(SLOTS - 1, -1, -1):
            @pl.when(step >= back)
            def _():
                finish(step - back, True)


def attention(chunk, rows, lens, hidden, cos_t, sin_t, s1, b1, wqkv, bqkv, wout, kt, vt, prev):
    per_sub = SUB // BB
    n_step = rows // BB
    first = chunk * rows // SUB
    vec = pl.BlockSpec((1024,), lambda i, s: (0,))
    hbm = pl.BlockSpec(memory_space=pl.ANY)
    in_specs = [
        pl.BlockSpec((SUB, 1024), lambda i, s: (first + i // per_sub, 0)),
        pl.BlockSpec((32, SUB), lambda i, s: (0, first + i // per_sub)),
        pl.BlockSpec((32, SUB), lambda i, s: (0, first + i // per_sub)),
        vec, vec, vec, hbm, hbm, hbm, hbm,
    ]
    args = [lens, hidden, cos_t, sin_t, s1, b1, bqkv, wqkv, wout, kt, vt]
    aliases = {}
    if prev is not None:
        in_specs += [hbm, hbm]
        aliases = {len(args): 1, len(args) + 1: 2}
        args += list(prev)
    return pl.pallas_call(
        functools.partial(attention_kernel, chunk * rows, int(prev is not None)),
        grid_spec=pltpu.PrefetchScalarGridSpec(
            num_scalar_prefetch=1, grid=(n_step,), in_specs=in_specs,
            out_specs=[pl.BlockSpec((SUB, 1024), lambda i, s: (i // per_sub, 0)), hbm, hbm],
            scratch_shapes=[
                pltpu.VMEM(wqkv.shape, BF), pltpu.VMEM(wout.shape, BF),
                pltpu.VMEM((SLOTS, BB, 4, 64, 128), BF), pltpu.VMEM((SLOTS, BB, 4, 64, 128), BF),
                pltpu.VMEM((2 * SUB * 8, 128), F32), pltpu.VMEM((256, SUB), F32), pltpu.VMEM((256, SUB), F32),
                pltpu.VMEM((BB * 8, 128), F32), pltpu.VMEM((BB * 8, 128), F32),
                pltpu.VMEM((2 * BB * 8, 128), F32), pltpu.VMEM((SUB, 512), BF),
                pltpu.SemaphoreType.DMA((2, SLOTS)), pltpu.SemaphoreType.DMA((2, SLOTS)), pltpu.SemaphoreType.DMA((2,))]),
        out_shape=[jax.ShapeDtypeStruct((rows, 1024), BF), jax.ShapeDtypeStruct(kt.shape, BF), jax.ShapeDtypeStruct(vt.shape, BF)],
        input_output_aliases=aliases,
        compiler_params=pltpu.CompilerParams(dimension_semantics=("arbitrary",), vmem_limit_bytes=40 * 1024 * 1024),
        cost_estimate=pl.CostEstimate(flops=rows * 20_000_000, bytes_accessed=rows * 262144, transcendentals=0),
        name="attention",
    )(*args)


def mid_kernel(hid_ref, one_ref, two_ref, bo_ref, s2_ref, b2_ref, x1_ref, h2_ref):
    attn = one_ref[...].astype(F32) + two_ref[...].astype(F32)
    x1 = (hid_ref[...].astype(F32) + attn + wide(bo_ref)).astype(BF)
    x1_ref[...] = x1
    h2_ref[...] = norm_rows(x1.astype(F32), wide(s2_ref), wide(b2_ref))


def middle(chunk, rows, hidden, one, two, b_out, s2, b2):
    tile = 128
    off = chunk * rows // tile
    vec = pl.BlockSpec((1024,), lambda i: (0,))
    blk = pl.BlockSpec((tile, 1024), lambda i: (i, 0))
    return pl.pallas_call(
        mid_kernel, grid=(rows // tile,),
        in_specs=[pl.BlockSpec((tile, 1024), lambda i: (off + i, 0)), blk, blk, vec, vec, vec],
        out_specs=[blk, blk],
        out_shape=[jax.ShapeDtypeStruct((rows, 1024), BF)] * 2,
        cost_estimate=pl.CostEstimate(flops=rows * 400_000, bytes_accessed=rows * 10240, transcendentals=0),
        name="middle",
    )(hidden, one, two, b_out, s2, b2)


def expert_kernel(rows, first_ref, x0, x1, x2, x3, i0, i1, i2, i3, wr_ref, wg_ref, wu_ref, wd_ref, o0, o1, o2, o3, acc_ref, gate_ref):
    e = pl.program_id(0)
    n_e = pl.num_programs(0)
    xs, ids, outs = (x0, x1, x2, x3), (i0, i1, i2, i3), (o0, o1, o2, o3)
    tile = min(rows, 256)

    @pl.when(e == 0)
    def _():
        for n in range(4):
            logit = lax.dot_general(wr_ref[...], xs[n][...], (((1,), (1,)), ((), ())), preferred_element_type=F32)
            eid = lax.broadcasted_iota(jnp.int32, (32, rows), 0)
            picked = eid == ids[n][0:1, :]
            for m in range(1, 8):
                picked = picked | (eid == ids[n][m:m + 1, :])
            logit = jnp.where(picked, logit, -jnp.inf)
            ex = jnp.exp(logit - jnp.max(logit, axis=0, keepdims=True))
            prob = (ex / jnp.sum(ex, axis=0, keepdims=True)).astype(BF).astype(F32)
            gate_ref[n * rows:(n + 1) * rows, :] = jnp.transpose(prob)

        acc_ref[...] = jnp.zeros_like(acc_ref)

    mine = first_ref[0] + e
    lane = lax.broadcasted_iota(jnp.int32, (tile, 32), 1)
    for n in range(4):
        for t in range(rows // tile):
            row = n * rows + t * tile
            x = xs[n][t * tile:(t + 1) * tile, :]
            gate = jnp.dot(x, wg_ref[0], preferred_element_type=F32)
            up = jnp.dot(x, wu_ref[0], preferred_element_type=F32)
            act = (gate * jax.nn.sigmoid(gate) * up).astype(BF)
            y = jnp.dot(act, wd_ref[0], preferred_element_type=F32)
            g_one = jnp.sum(jnp.where(lane == mine, gate_ref[row:row + tile, :], 0.0), axis=-1, keepdims=True)
            acc_ref[row:row + tile, :] += g_one * y

    @pl.when(e == n_e - 1)
    def _():
        for n in range(4):
            outs[n][...] = acc_ref[n * rows:(n + 1) * rows, :].astype(BF)


def experts(rows, first, xs, ids, wr_t, wg, wu, wd):
    n_e = wg.shape[0]
    full = lambda shape: pl.BlockSpec(shape, lambda e, s: (0,) * len(shape), pipeline_mode=pl.Buffered(1))
    wspec = lambda a: pl.BlockSpec((1,) + a.shape[1:], lambda e, s: (e, 0, 0))
    return pl.pallas_call(
        functools.partial(expert_kernel, rows),
        grid_spec=pltpu.PrefetchScalarGridSpec(
            num_scalar_prefetch=1, grid=(n_e,),
            in_specs=[full((rows, 1024))] * 4 + [full((8, rows))] * 4 + [full((32, 1024)), wspec(wg), wspec(wu), wspec(wd)],
            out_specs=[full((rows, 1024))] * 4,
            scratch_shapes=[pltpu.VMEM((4 * rows, 1024), F32), pltpu.VMEM((4 * rows, 32), F32)]),
        out_shape=[jax.ShapeDtypeStruct((rows, 1024), BF)] * 4,
        compiler_params=pltpu.CompilerParams(dimension_semantics=("arbitrary",), vmem_limit_bytes=VMEM_LIMIT),
        cost_estimate=pl.CostEstimate(flops=rows * 4 * n_e * 1_600_000, bytes_accessed=14_000_000, transcendentals=0),
        name="experts",
    )(first, *xs, *ids, wr_t, wg, wu, wd)


def finish_kernel(x1_ref, one_ref, two_ref, *rest):
    moe = one_ref[...].astype(F32) + two_ref[...].astype(F32)
    rest[-1][...] = (x1_ref[...].astype(F32) + moe).astype(BF)


def finish_rows(chunk, n_batch, x1, one, two, prev):
    rows = x1.shape[0]
    blk = pl.BlockSpec((rows, 1024), lambda i: (0, 0))
    more = [] if prev is None else [prev]
    return pl.pallas_call(
        finish_kernel, grid=(1,),
        in_specs=[blk] * 3 + [pl.BlockSpec(memory_space=pl.ANY)] * len(more),
        out_specs=pl.BlockSpec((rows, 1024), lambda i: (chunk, 0)),
        out_shape=jax.ShapeDtypeStruct((n_batch, 1024), BF),
        input_output_aliases={3: 0} if more else {},
        cost_estimate=pl.CostEstimate(flops=rows * 100_000, bytes_accessed=rows * 8192, transcendentals=0),
        name="finish",
    )(x1, one, two, *more)


def add_rows(one, two):
    return (one.astype(F32) + two.astype(F32)).astype(BF)


def solution(mesh):
    n_ep = mesh.shape['ep']
    token_rows = P(('dp', 'ep'), None)
    token_vec = P(('dp', 'ep'))
    cache_spec = P(('dp', 'ep'), None, 'tp', None)
    expert_in = P('ep', None, 'tp')
    expert_down = P('ep', 'tp', None)

    def swap_ep(x, bit):
        return lax.ppermute(x, 'ep', [(d, d ^ bit) for d in range(n_ep)])

    def swap_tp(x):
        return lax.ppermute(x, 'tp', [(0, 1), (1, 0)])

    def device_step(hidden, seq_lens, rope_cos, rope_sin, ln1_scale, ln1_bias, w_qkv, b_qkv, w_out, b_out, k_cache, v_cache, ln2_scale, ln2_bias, w_router, expert_ids, w_gate, w_up, w_down):
        n_batch = hidden.shape[0]
        rows = n_batch // CHUNKS
        kt, vt = (jnp.transpose(c, (0, 2, 3, 1)) for c in (k_cache, v_cache))
        ids_far = swap_ep(expert_ids.T, 2)
        ids_near = swap_ep(expert_ids.T, 1)
        ids = [expert_ids.T, ids_near, ids_far, swap_ep(ids_far, 1)]
        first = (lax.axis_index('ep') * w_gate.shape[0]).astype(jnp.int32).reshape(1)
        prev, out, x1s, h2s = None, None, [], []
        for c in range(CHUNKS):
            part, *prev = attention(c, rows, seq_lens, hidden, rope_cos.T, rope_sin.T, ln1_scale, ln1_bias, w_qkv, b_qkv, w_out, kt, vt, prev)
            other = swap_tp(part)
            x1, h2 = middle(c, rows, hidden, part, other, b_out, ln2_scale, ln2_bias)
            far = swap_ep(h2, 2)
            near = swap_ep(h2, 1)
            both = swap_ep(far, 1)
            x1s.append(x1)
            h2s.append([h2, near, far, both])
        for c in range(CHUNKS):
            o = experts(rows, first, h2s[c], [a[:, c * rows:(c + 1) * rows] for a in ids], w_router.T, w_gate, w_up, w_down)
            from_near = swap_ep(o[1], 1)
            from_pass = swap_ep(o[3], 1)
            far = add_rows(o[2], from_pass)
            from_far = swap_ep(far, 2)
            near = add_rows(o[0], from_near)
            total = add_rows(near, from_far)
            other = swap_tp(total)
            out = finish_rows(c, n_batch, x1s[c], total, other, out)
        return out, *(jnp.transpose(c, (0, 3, 1, 2)) for c in prev)

    in_specs = (token_rows, token_vec, token_rows, token_rows, P(), P(), P(None, 'tp'), P('tp'), P('tp', None), P(), cache_spec, cache_spec, P(), P(), P(), token_rows, expert_in, expert_in, expert_down)
    return jax.shard_map(device_step, mesh=mesh, in_specs=in_specs, out_specs=(token_rows, cache_spec, cache_spec), check_vma=False)
```

```python
import functools

import jax
import jax.numpy as jnp
from jax import lax
from jax.experimental import pallas as pl
from jax.experimental.pallas import tpu as pltpu
from jax.sharding import PartitionSpec as P

EPS = 1e-5
BF = jnp.bfloat16
F32 = jnp.float32
CHUNKS = 4
SUB = 128
BB = 16
TILE = 512
WIDE = 1024 + 128
SLOTS = 8
AHEAD = 5
VMEM_LIMIT = 60 * 1024 * 1024


def norm_rows(x, scale, bias):
    mean = jnp.mean(x, axis=-1, keepdims=True)
    cen = x - mean
    var = jnp.mean(cen * cen, axis=-1, keepdims=True)
    return (cen * lax.rsqrt(var + EPS) * scale + bias).astype(BF)


def wide(ref):
    return ref[...].astype(F32).reshape(1, -1)


def attention_kernel(form, base_row, has_prev, len_ref, hid_ref, cos_ref, sin_ref, s1_ref, b1_ref, bqkv_ref, wqkv_hbm, wout_hbm, k_hbm, v_hbm, *rest):
    part_ref, ko_hbm, vo_hbm = rest[2 * has_prev:2 * has_prev + 3]
    wqkv_ref, wout_ref, kb_ref, vb_ref, qs_ref, kt_ref, vt_ref, sc_ref, pr_ref, cx_ref, ctx_ref, in_sem, out_sem, w_sem = rest[2 * has_prev + 3:]
    step = pl.program_id(0)
    n_step = pl.num_programs(0)
    per_sub = SUB // BB
    j = lax.rem(step, per_sub)
    lane = lax.broadcasted_iota(jnp.int32, (SUB, 128), 1)
    low = lane < 64

    def moves(s, out):
        slot = lax.rem(s, SLOTS)
        src = pl.ds(base_row + s * BB, BB)
        pairs = ((k_hbm, kb_ref, ko_hbm, 0), (v_hbm, vb_ref, vo_hbm, 1))
        if out:
            return [(pltpu.make_async_copy(buf.at[slot], dst.at[src], out_sem.at[t, slot]), t) for _, buf, dst, t in pairs]
        return [(pltpu.make_async_copy(hbm.at[src], buf.at[slot], in_sem.at[t, slot]), t) for hbm, buf, _, t in pairs]

    def begin(s, out):
        for copy, t in moves(s, out):
            copy.start(priority=t)

    def finish(s, out):
        for copy, _ in moves(s, out):
            copy.wait()

    load_qkv = pltpu.make_async_copy(wqkv_hbm, wqkv_ref, w_sem.at[0])
    load_out = pltpu.make_async_copy(wout_hbm, wout_ref, w_sem.at[1])

    @pl.when(step == 0)
    def _():
        load_qkv.start()
        for s in range(AHEAD):
            begin(s, False)
        load_out.start()
        load_qkv.wait()

    @pl.when(j == 0)
    def _():
        normed = norm_rows(hid_ref[...].astype(F32), wide(s1_ref), wide(b1_ref))
        qkv = jnp.dot(normed, wqkv_ref[...], preferred_element_type=F32) + wide(bqkv_ref)
        qkv = qkv.astype(BF).astype(F32)
        col = [qkv[:, m * 128:(m + 1) * 128] for m in range(8)]
        rol = [pltpu.roll(c, 64, 1) for c in col]

        def first(a, b):
            return jnp.where(low, col[a], rol[b])

        def second(a, b):
            return jnp.where(low, rol[a], col[b])

        cos_t, sin_t = cos_ref[...], sin_ref[...]
        cos = jnp.transpose(jnp.concatenate([cos_t] * 4, axis=0))
        sin = jnp.transpose(jnp.concatenate([-sin_t, sin_t] * 2, axis=0))

        def rope(x):
            other = jnp.where(lane % 64 < 32, pltpu.roll(x, 96, 1), pltpu.roll(x, 32, 1))
            return (x * cos + other * sin).astype(BF).astype(F32)

        for h in range(2):
            q0 = rope(first(4 * h, 4 * h + 2))
            q1 = rope(second(4 * h, 4 * h + 2))
            kk = rope(first(4 * h + 1, 4 * h + 3))
            vv = second(4 * h + 1, 4 * h + 3)
            kt_ref[h * 128:(h + 1) * 128, :] = jnp.transpose(kk).astype(BF)
            vt_ref[h * 128:(h + 1) * 128, :] = jnp.transpose(vv).astype(BF)
            for r in range(8):
                src = q0 if r % 2 == 0 else q1
                if r // 4 == h:
                    src = jnp.where(low if (r // 2) % 2 == 0 else ~low, src, 0.0)
                else:
                    src = jnp.zeros_like(src)
                qs_ref[pl.ds(h * SUB * 8 + r, SUB, stride=8), :] = src

    slot = lax.rem(step, SLOTS)
    finish(step, False)
    shift = lax.rem(SUB - j * BB, SUB)
    kt, vt = None, None
    if form == "A":
        kt = pltpu.roll(kt_ref[...], shift, 1)
        vt = pltpu.roll(vt_ref[...], shift, 1)

    def pick(moved, ref, b, pos):
        if form == "A":
            return jnp.broadcast_to(moved[:, b:b + 1], (256, 128))
        return pltpu.roll(ref[...], lax.rem(pos + shift + SUB - b, SUB), 1)

    lane8 = lax.broadcasted_iota(jnp.int32, (8, 128), 1)
    lane256 = lax.broadcasted_iota(jnp.int16, (256, 128), 1)
    row0 = pl.multiple_of(j * BB * 8, BB * 8)
    base = base_row + step * BB
    for b in range(BB):
        pos = len_ref[base + b]
        k_old = kb_ref[slot, b].reshape(256, 128)
        k_new = jnp.where(lane256 == pos.astype(jnp.int16), pick(kt, kt_ref, b, pos), k_old)
        kb_ref[slot, b] = k_new.reshape(4, 64, 128)
        q_one = jnp.concatenate([qs_ref[pl.ds(row0 + h * SUB * 8 + b * 8, 8), :] for h in range(2)], axis=1).astype(BF)
        s_one = jnp.dot(q_one, k_new, preferred_element_type=F32) * 0.125
        sc_ref[b * 8:(b + 1) * 8, :] = jnp.where(lane8 <= pos, s_one, -jnp.inf)
    s_all = sc_ref[...]
    e_all = jnp.exp(s_all - jnp.max(s_all, axis=-1, keepdims=True))
    pr_ref[...] = e_all / jnp.sum(e_all, axis=-1, keepdims=True)
    for b in range(BB):
        pos = len_ref[base + b]
        v_old = vb_ref[slot, b].reshape(256, 128)
        v_new = jnp.where(lane256 == pos.astype(jnp.int16), pick(vt, vt_ref, b, pos), v_old)
        vb_ref[slot, b] = v_new.reshape(4, 64, 128)
        p_one = pr_ref[b * 8:(b + 1) * 8, :].astype(BF)
        c_one = lax.dot_general(p_one, v_new, (((1,), (1,)), ((), ())), preferred_element_type=F32)
        cx_ref[b * 8:(b + 1) * 8, :] = c_one[:, :128]
        cx_ref[BB * 8 + b * 8:BB * 8 + (b + 1) * 8, :] = c_one[:, 128:]
    low_b = lax.broadcasted_iota(jnp.int32, (BB, 128), 1) < 64
    for h in range(2):
        for g in range(2):
            r = 4 * h + 2 * g
            one = cx_ref[pl.ds(h * BB * 8 + r, BB, stride=8), :]
            two = cx_ref[pl.ds(h * BB * 8 + r + 1, BB, stride=8), :]
            if g == 0:
                both = jnp.where(low_b, one, pltpu.roll(two, 64, 1))
            else:
                both = jnp.where(low_b, pltpu.roll(one, 64, 1), two)
            ctx_ref[pl.ds(pl.multiple_of(j * BB, BB), BB), (2 * h + g) * 128:(2 * h + g + 1) * 128] = both.astype(BF)

    begin(step, True)

    @pl.when(step + AHEAD < n_step)
    def _():
        @pl.when(step + AHEAD >= SLOTS)
        def _():
            finish(step + AHEAD - SLOTS, True)

        begin(step + AHEAD, False)

    @pl.when(step == per_sub - 1)
    def _():
        load_out.wait()

    @pl.when(j == per_sub - 1)
    def _():
        part_ref[...] = jnp.dot(ctx_ref[...], wout_ref[...], preferred_element_type=F32).astype(BF)

    @pl.when(step == n_step - 1)
    def _():
        for back in range(SLOTS - 1, -1, -1):
            @pl.when(step >= back)
            def _():
                finish(step - back, True)


def attention(chunk, rows, lens, hidden, cos_t, sin_t, s1, b1, wqkv, bqkv, wout, kt, vt, prev):
    per_sub = SUB // BB
    n_step = rows // BB
    first = chunk * rows // SUB
    vec = pl.BlockSpec((1024,), lambda i, s: (0,))
    hbm = pl.BlockSpec(memory_space=pl.ANY)
    in_specs = [
        pl.BlockSpec((SUB, 1024), lambda i, s: (first + i // per_sub, 0)),
        pl.BlockSpec((32, SUB), lambda i, s: (0, first + i // per_sub)),
        pl.BlockSpec((32, SUB), lambda i, s: (0, first + i // per_sub)),
        vec, vec, vec, hbm, hbm, hbm, hbm,
    ]
    args = [lens, hidden, cos_t, sin_t, s1, b1, bqkv, wqkv, wout, kt, vt]
    aliases = {}
    if prev is not None:
        in_specs += [hbm, hbm]
        aliases = {len(args): 1, len(args) + 1: 2}
        args += list(prev)
    return pl.pallas_call(
        functools.partial(attention_kernel, 'AB'[chunk >= 2], chunk * rows, int(prev is not None)),
        grid_spec=pltpu.PrefetchScalarGridSpec(
            num_scalar_prefetch=1, grid=(n_step,), in_specs=in_specs,
            out_specs=[pl.BlockSpec((SUB, 1024), lambda i, s: (i // per_sub, 0)), hbm, hbm],
            scratch_shapes=[
                pltpu.VMEM(wqkv.shape, BF), pltpu.VMEM(wout.shape, BF),
                pltpu.VMEM((SLOTS, BB, 4, 64, 128), BF), pltpu.VMEM((SLOTS, BB, 4, 64, 128), BF),
                pltpu.VMEM((2 * SUB * 8, 128), F32), pltpu.VMEM((256, SUB), BF), pltpu.VMEM((256, SUB), BF),
                pltpu.VMEM((BB * 8, 128), F32), pltpu.VMEM((BB * 8, 128), F32),
                pltpu.VMEM((2 * BB * 8, 128), F32), pltpu.VMEM((SUB, 512), BF),
                pltpu.SemaphoreType.DMA((2, SLOTS)), pltpu.SemaphoreType.DMA((2, SLOTS)), pltpu.SemaphoreType.DMA((2,))]),
        out_shape=[jax.ShapeDtypeStruct((rows, 1024), BF), jax.ShapeDtypeStruct(kt.shape, BF), jax.ShapeDtypeStruct(vt.shape, BF)],
        input_output_aliases=aliases,
        compiler_params=pltpu.CompilerParams(dimension_semantics=("arbitrary",), vmem_limit_bytes=VMEM_LIMIT),
        cost_estimate=pl.CostEstimate(flops=rows * 20_000_000, bytes_accessed=rows * 262144, transcendentals=0),
        name="attention",
    )(*args)


def mid_kernel(hid_ref, one_ref, two_ref, bo_ref, s2_ref, b2_ref, wr_ref, ids_ref, x1_ref, h2_ref):
    attn = one_ref[...].astype(F32) + two_ref[...].astype(F32)
    x1 = (hid_ref[...].astype(F32) + attn + wide(bo_ref)).astype(BF)
    x1_ref[...] = x1
    h2 = norm_rows(x1.astype(F32), wide(s2_ref), wide(b2_ref))
    h2_ref[:, :1024] = h2
    rows = h2.shape[0]
    logit = lax.dot_general(wr_ref[...], h2, (((1,), (1,)), ((), ())), preferred_element_type=F32)
    eid = lax.broadcasted_iota(jnp.int32, (32, rows), 0)
    picked = eid == ids_ref[0:1, :]
    for m in range(1, 8):
        picked = picked | (eid == ids_ref[m:m + 1, :])
    logit = jnp.where(picked, logit, -jnp.inf)
    ex = jnp.exp(logit - jnp.max(logit, axis=0, keepdims=True))
    prob = ex / jnp.sum(ex, axis=0, keepdims=True)
    full = jnp.concatenate([prob, jnp.zeros((96, rows), F32)], axis=0)
    h2_ref[:, 1024:] = jnp.transpose(full).astype(BF)


def middle(chunk, rows, hidden, one, two, b_out, s2, b2, wr_t, ids):
    vec = pl.BlockSpec((1024,), lambda i: (0,))
    blk = pl.BlockSpec((rows, 1024), lambda i: (0, 0))
    return pl.pallas_call(
        mid_kernel, grid=(1,),
        in_specs=[pl.BlockSpec((rows, 1024), lambda i: (chunk, 0)), blk, blk, vec, vec, vec,
                  pl.BlockSpec((32, 1024), lambda i: (0, 0)), pl.BlockSpec((8, rows), lambda i: (0, chunk))],
        out_specs=[blk, pl.BlockSpec((rows, WIDE), lambda i: (0, 0))],
        out_shape=[jax.ShapeDtypeStruct((rows, 1024), BF), jax.ShapeDtypeStruct((rows, WIDE), BF)],
        compiler_params=pltpu.CompilerParams(vmem_limit_bytes=VMEM_LIMIT),
        cost_estimate=pl.CostEstimate(flops=rows * 400_000, bytes_accessed=rows * 10240, transcendentals=0),
        name="middle",
    )(hidden, one, two, b_out, s2, b2, wr_t, ids)


def expert_kernel(rows, tile, first_ref, x0, x1, x2, x3, wg_ref, wu_ref, wd_ref, o0, o1, o2, o3, acc_ref, gate_ref, x_ref):
    e = pl.program_id(0)
    n_e = pl.num_programs(0)
    xs, outs = (x0, x1, x2, x3), (o0, o1, o2, o3)

    @pl.when(e == 0)
    def _():
        for n in range(4):
            gate_ref[n * rows:(n + 1) * rows, :] = xs[n][:, 1024:].astype(F32)
            x_ref[n * rows:(n + 1) * rows, :] = xs[n][:, :1024]
        acc_ref[...] = jnp.zeros_like(acc_ref)

    mine = first_ref[0] + e
    lane = lax.broadcasted_iota(jnp.int32, (tile, 128), 1)
    for row in range(0, 4 * rows, tile):
        x = x_ref[row:row + tile, :]
        gate = jnp.dot(x, wg_ref[0], preferred_element_type=F32)
        up = jnp.dot(x, wu_ref[0], preferred_element_type=F32)
        act = (gate * jax.nn.sigmoid(gate) * up).astype(BF)
        y = jnp.dot(act, wd_ref[0], preferred_element_type=F32)
        g_one = jnp.sum(jnp.where(lane == mine, gate_ref[row:row + tile, :], 0.0), axis=-1, keepdims=True)
        acc_ref[row:row + tile, :] += g_one * y

    @pl.when(e == n_e - 1)
    def _():
        for n in range(4):
            outs[n][...] = acc_ref[n * rows:(n + 1) * rows, :].astype(BF)


def experts(rows, tile, first, xs, wg, wu, wd):
    n_e = wg.shape[0]
    full = lambda shape: pl.BlockSpec(shape, lambda e, s: (0,) * len(shape), pipeline_mode=pl.Buffered(1))
    wspec = lambda a: pl.BlockSpec((1,) + a.shape[1:], lambda e, s: (e, 0, 0))
    return pl.pallas_call(
        functools.partial(expert_kernel, rows, tile),
        grid_spec=pltpu.PrefetchScalarGridSpec(
            num_scalar_prefetch=1, grid=(n_e,),
            in_specs=[full((rows, WIDE))] * 4 + [wspec(wg), wspec(wu), wspec(wd)],
            out_specs=[full((rows, 1024))] * 4,
            scratch_shapes=[pltpu.VMEM((4 * rows, 1024), F32), pltpu.VMEM((4 * rows, 128), F32), pltpu.VMEM((4 * rows, 1024), BF)]),
        out_shape=[jax.ShapeDtypeStruct((rows, 1024), BF)] * 4,
        compiler_params=pltpu.CompilerParams(dimension_semantics=("arbitrary",), vmem_limit_bytes=VMEM_LIMIT),
        cost_estimate=pl.CostEstimate(flops=rows * 4 * n_e * 1_600_000, bytes_accessed=14_000_000, transcendentals=0),
        name="experts",
    )(first, *xs, wg, wu, wd)


def finish_kernel(count, *refs):
    rows = refs[0].shape[0]
    for m in range(count):
        x1, one, two = refs[3 * m:3 * m + 3]
        moe = one[...].astype(F32) + two[...].astype(F32)
        refs[-1][m * rows:(m + 1) * rows, :] = (x1[...].astype(F32) + moe).astype(BF)


def finish_rows(first, n_batch, triples, prev):
    count = len(triples)
    rows = triples[0][0].shape[0]
    blk = pl.BlockSpec((rows, 1024), lambda i: (0, 0))
    more = [] if prev is None else [prev]
    return pl.pallas_call(
        functools.partial(finish_kernel, count), grid=(1,),
        in_specs=[blk] * (3 * count) + [pl.BlockSpec(memory_space=pl.ANY)] * len(more),
        out_specs=pl.BlockSpec((count * rows, 1024), lambda i: (first // count, 0)),
        out_shape=jax.ShapeDtypeStruct((n_batch, 1024), BF),
        input_output_aliases={3 * count: 0} if more else {},
        compiler_params=pltpu.CompilerParams(vmem_limit_bytes=VMEM_LIMIT),
        cost_estimate=pl.CostEstimate(flops=rows * count * 100_000, bytes_accessed=rows * count * 8192, transcendentals=0),
        name="finish",
    )(*[a for t in triples for a in t], *more)


def add_rows(*parts):
    total = parts[0].astype(F32)
    for one in parts[1:]:
        total = total + one.astype(F32)
    return total.astype(BF)


def solution(mesh):
    n_ep = mesh.shape['ep']
    token_rows = P(('dp', 'ep'), None)
    token_vec = P(('dp', 'ep'))
    cache_spec = P(('dp', 'ep'), None, 'tp', None)
    expert_in = P('ep', None, 'tp')
    expert_down = P('ep', 'tp', None)

    def swap_ep(x, bit):
        return lax.ppermute(x, 'ep', [(d, d ^ bit) for d in range(n_ep)])

    def swap_tp(x):
        return lax.ppermute(x, 'tp', [(0, 1), (1, 0)])

    def device_step(hidden, seq_lens, rope_cos, rope_sin, ln1_scale, ln1_bias, w_qkv, b_qkv, w_out, b_out, k_cache, v_cache, ln2_scale, ln2_bias, w_router, expert_ids, w_gate, w_up, w_down):
        n_batch = hidden.shape[0]
        rows = n_batch // CHUNKS
        kt, vt = (jnp.transpose(c, (0, 2, 3, 1)) for c in (k_cache, v_cache))
        first = (lax.axis_index('ep') * w_gate.shape[0]).astype(jnp.int32).reshape(1)
        prev, out, x1s, h2s, sums = None, None, [], [], []
        for c in range(CHUNKS):
            part, *prev = attention(c, rows, seq_lens, hidden, rope_cos.T, rope_sin.T, ln1_scale, ln1_bias, w_qkv, b_qkv, w_out, kt, vt, prev)
            other = swap_tp(part)
            x1, h2 = middle(c, rows, hidden, part, other, b_out, ln2_scale, ln2_bias, w_router.T, expert_ids.T)
            far = swap_ep(h2, 2)
            near = swap_ep(h2, 1)
            both = swap_ep(far, 1)
            x1s.append(x1)
            h2s.append([h2, near, far, both])
        for c in range(CHUNKS):
            o = experts(rows, TILE, first, h2s[c], w_gate, w_up, w_down)
            from_near = swap_ep(o[1], 1)
            if c < CHUNKS - 1:
                from_far = swap_ep(o[2], 2)
                from_cross = swap_ep(o[3], 3)
                total = add_rows(o[0], from_near, from_far, from_cross)
            else:
                from_cross = swap_ep(o[3], 1)
                far = add_rows(o[2], from_cross)
                from_far = swap_ep(far, 2)
                total = add_rows(add_rows(o[0], from_near), from_far)
            sums.append((x1s[c], total, swap_tp(total)))
        out = finish_rows(0, n_batch, sums[:-1], None)
        out = finish_rows(CHUNKS - 1, n_batch, sums[-1:], out)
        return out, *(jnp.transpose(c, (0, 3, 1, 2)) for c in prev)

    in_specs = (token_rows, token_vec, token_rows, token_rows, P(), P(), P(None, 'tp'), P('tp'), P('tp', None), P(), cache_spec, cache_spec, P(), P(), P(), token_rows, expert_in, expert_in, expert_down)
    return jax.shard_map(device_step, mesh=mesh, in_specs=in_specs, out_specs=(token_rows, cache_spec, cache_spec), check_vma=False)
```

```python
import functools

import jax
import jax.numpy as jnp
from jax import lax
from jax.experimental import pallas as pl
from jax.experimental.pallas import tpu as pltpu
from jax.sharding import PartitionSpec as P

EPS = 1e-5
BF = jnp.bfloat16
F32 = jnp.float32
CHUNKS = 4
SUB = 128
BB = 16
WIDE = 1024 + 128
SLOTS = 8
AHEAD = 5
VMEM_LIMIT = 60 * 1024 * 1024


def norm_rows(x, scale, bias):
    mean = jnp.mean(x, axis=-1, keepdims=True)
    cen = x - mean
    var = jnp.mean(cen * cen, axis=-1, keepdims=True)
    return (cen * lax.rsqrt(var + EPS) * scale + bias).astype(BF)


def wide(ref):
    return ref[...].astype(F32).reshape(1, -1)


def attention_kernel(base_row, has_prev, len_ref, hid_ref, cos_ref, sin_ref, s1_ref, b1_ref, bqkv_ref, wqkv_hbm, wout_hbm, k_hbm, v_hbm, *rest):
    part_ref, ko_hbm, vo_hbm = rest[2 * has_prev:2 * has_prev + 3]
    wqkv_ref, wout_ref, kb_ref, vb_ref, qs_ref, kt_ref, vt_ref, sc_ref, pr_ref, cx_ref, ctx_ref, in_sem, out_sem, w_sem = rest[2 * has_prev + 3:]
    step = pl.program_id(0)
    n_step = pl.num_programs(0)
    per_sub = SUB // BB
    j = lax.rem(step, per_sub)
    lane = lax.broadcasted_iota(jnp.int32, (SUB, 128), 1)
    low = lane < 64

    def moves(s, out):
        slot = lax.rem(s, SLOTS)
        src = pl.ds(base_row + s * BB, BB)
        pairs = ((k_hbm, kb_ref, ko_hbm, 0), (v_hbm, vb_ref, vo_hbm, 1))
        if out:
            return [(pltpu.make_async_copy(buf.at[slot], dst.at[src], out_sem.at[t, slot]), t) for _, buf, dst, t in pairs]
        return [(pltpu.make_async_copy(hbm.at[src], buf.at[slot], in_sem.at[t, slot]), t) for hbm, buf, _, t in pairs]

    def begin(s, out):
        for copy, t in moves(s, out):
            copy.start(priority=t)

    def finish(s, out):
        for copy, _ in moves(s, out):
            copy.wait()

    load_qkv = pltpu.make_async_copy(wqkv_hbm, wqkv_ref, w_sem.at[0])
    load_out = pltpu.make_async_copy(wout_hbm, wout_ref, w_sem.at[1])

    @pl.when(step == 0)
    def _():
        load_qkv.start()
        for s in range(AHEAD):
            begin(s, False)
        load_out.start()
        load_qkv.wait()

    @pl.when(j == 0)
    def _():
        normed = norm_rows(hid_ref[...].astype(F32), wide(s1_ref), wide(b1_ref))
        qkv = jnp.dot(normed, wqkv_ref[...], preferred_element_type=F32) + wide(bqkv_ref)
        qkv = qkv.astype(BF).astype(F32)
        col = [qkv[:, m * 128:(m + 1) * 128] for m in range(8)]
        rol = [pltpu.roll(c, 64, 1) for c in col]

        def first(a, b):
            return jnp.where(low, col[a], rol[b])

        def second(a, b):
            return jnp.where(low, rol[a], col[b])

        cos_t, sin_t = cos_ref[...], sin_ref[...]
        cos = jnp.transpose(jnp.concatenate([cos_t] * 4, axis=0))
        sin = jnp.transpose(jnp.concatenate([-sin_t, sin_t] * 2, axis=0))

        def rope(x):
            other = jnp.where(lane % 64 < 32, pltpu.roll(x, 96, 1), pltpu.roll(x, 32, 1))
            return (x * cos + other * sin).astype(BF).astype(F32)

        for h in range(2):
            q0 = rope(first(4 * h, 4 * h + 2))
            q1 = rope(second(4 * h, 4 * h + 2))
            kk = rope(first(4 * h + 1, 4 * h + 3))
            vv = second(4 * h + 1, 4 * h + 3)
            kt_ref[h * 128:(h + 1) * 128, :] = jnp.transpose(kk)
            vt_ref[h * 128:(h + 1) * 128, :] = jnp.transpose(vv)
            for r in range(8):
                src = q0 if r % 2 == 0 else q1
                if r // 4 == h:
                    src = jnp.where(low if (r // 2) % 2 == 0 else ~low, src, 0.0)
                else:
                    src = jnp.zeros_like(src)
                qs_ref[pl.ds(h * SUB * 8 + r, SUB, stride=8), :] = src

    slot = lax.rem(step, SLOTS)
    finish(step, False)
    shift = lax.rem(SUB - j * BB, SUB)
    kt = pltpu.roll(kt_ref[...], shift, 1)
    vt = pltpu.roll(vt_ref[...], shift, 1)
    lane8 = lax.broadcasted_iota(jnp.int32, (8, 128), 1)
    lane256 = lax.broadcasted_iota(jnp.int32, (256, 128), 1)
    row0 = pl.multiple_of(j * BB * 8, BB * 8)
    base = base_row + step * BB

    def placed(buf, cols, b):
        pos = len_ref[base + b]
        old = buf[slot, b].reshape(256, 128).astype(F32)
        new = jnp.where(lane256 == pos, cols[:, b:b + 1], old).astype(BF)
        buf[slot, b] = new.reshape(4, 64, 128)
        return pos, new

    for b in range(BB):
        pos, k_new = placed(kb_ref, kt, b)
        q_one = jnp.concatenate([qs_ref[pl.ds(row0 + h * SUB * 8 + b * 8, 8), :] for h in range(2)], axis=1).astype(BF)
        s_one = jnp.dot(q_one, k_new, preferred_element_type=F32) * 0.125
        sc_ref[b * 8:(b + 1) * 8, :] = jnp.where(lane8 <= pos, s_one, -jnp.inf)
    s_all = sc_ref[...]
    e_all = jnp.exp(s_all - jnp.max(s_all, axis=-1, keepdims=True))
    pr_ref[...] = e_all / jnp.sum(e_all, axis=-1, keepdims=True)
    for b in range(BB):
        _, v_new = placed(vb_ref, vt, b)
        p_one = pr_ref[b * 8:(b + 1) * 8, :].astype(BF)
        c_one = lax.dot_general(p_one, v_new, (((1,), (1,)), ((), ())), preferred_element_type=F32)
        cx_ref[b * 8:(b + 1) * 8, :] = c_one[:, :128]
        cx_ref[BB * 8 + b * 8:BB * 8 + (b + 1) * 8, :] = c_one[:, 128:]
    low_b = lax.broadcasted_iota(jnp.int32, (BB, 128), 1) < 64
    for h in range(2):
        for g in range(2):
            r = 4 * h + 2 * g
            one = cx_ref[pl.ds(h * BB * 8 + r, BB, stride=8), :]
            two = cx_ref[pl.ds(h * BB * 8 + r + 1, BB, stride=8), :]
            if g == 0:
                both = jnp.where(low_b, one, pltpu.roll(two, 64, 1))
            else:
                both = jnp.where(low_b, pltpu.roll(one, 64, 1), two)
            ctx_ref[pl.ds(pl.multiple_of(j * BB, BB), BB), (2 * h + g) * 128:(2 * h + g + 1) * 128] = both.astype(BF)

    begin(step, True)

    @pl.when(step + AHEAD < n_step)
    def _():
        @pl.when(step + AHEAD >= SLOTS)
        def _():
            finish(step + AHEAD - SLOTS, True)
        begin(step + AHEAD, False)

    @pl.when(step == per_sub - 1)
    def _():
        load_out.wait()

    @pl.when(j == per_sub - 1)
    def _():
        part_ref[...] = jnp.dot(ctx_ref[...], wout_ref[...], preferred_element_type=F32).astype(BF)

    @pl.when(step == n_step - 1)
    def _():
        for back in range(SLOTS - 1, -1, -1):
            @pl.when(step >= back)
            def _():
                finish(step - back, True)


def attention(chunk, rows, lens, hidden, cos_t, sin_t, s1, b1, wqkv, bqkv, wout, kt, vt, prev):
    per_sub = SUB // BB
    n_step = rows // BB
    first = chunk * rows // SUB
    vec = pl.BlockSpec((1024,), lambda i, s: (0,))
    hbm = pl.BlockSpec(memory_space=pl.ANY)
    in_specs = [
        pl.BlockSpec((SUB, 1024), lambda i, s: (first + i // per_sub, 0)),
        pl.BlockSpec((32, SUB), lambda i, s: (0, first + i // per_sub)),
        pl.BlockSpec((32, SUB), lambda i, s: (0, first + i // per_sub)),
        vec, vec, vec, hbm, hbm, hbm, hbm,
    ]
    args = [lens, hidden, cos_t, sin_t, s1, b1, bqkv, wqkv, wout, kt, vt]
    aliases = {}
    if prev is not None:
        in_specs += [hbm, hbm]
        aliases = {len(args): 1, len(args) + 1: 2}
        args += list(prev)
    return pl.pallas_call(
        functools.partial(attention_kernel, chunk * rows, int(prev is not None)),
        grid_spec=pltpu.PrefetchScalarGridSpec(
            num_scalar_prefetch=1, grid=(n_step,), in_specs=in_specs,
            out_specs=[pl.BlockSpec((SUB, 1024), lambda i, s: (i // per_sub, 0)), hbm, hbm],
            scratch_shapes=[
                pltpu.VMEM(wqkv.shape, BF), pltpu.VMEM(wout.shape, BF),
                pltpu.VMEM((SLOTS, BB, 4, 64, 128), BF), pltpu.VMEM((SLOTS, BB, 4, 64, 128), BF),
                pltpu.VMEM((2 * SUB * 8, 128), F32), pltpu.VMEM((256, SUB), F32), pltpu.VMEM((256, SUB), F32),
                pltpu.VMEM((BB * 8, 128), F32), pltpu.VMEM((BB * 8, 128), F32),
                pltpu.VMEM((2 * BB * 8, 128), F32), pltpu.VMEM((SUB, 512), BF),
                pltpu.SemaphoreType.DMA((2, SLOTS)), pltpu.SemaphoreType.DMA((2, SLOTS)), pltpu.SemaphoreType.DMA((2,))]),
        out_shape=[jax.ShapeDtypeStruct((rows, 1024), BF), jax.ShapeDtypeStruct(kt.shape, BF), jax.ShapeDtypeStruct(vt.shape, BF)],
        input_output_aliases=aliases,
        compiler_params=pltpu.CompilerParams(dimension_semantics=("arbitrary",), vmem_limit_bytes=VMEM_LIMIT),
        cost_estimate=pl.CostEstimate(flops=rows * 20_000_000, bytes_accessed=rows * 262144, transcendentals=0),
        name="attention",
    )(*args)


PART, NEAR, FAR, PASS, BACK1, BACK3, BACKX, BACKY = range(8)


def moe_kernel(part_ref, hid_ref, bo_ref, s2_ref, b2_ref, wr_ref, ids_ref, wg_hbm, wu_hbm, wd_hbm, out_ref,
               other, x1, xb, wg, wu, wd, acc, ob, rb, fb, rf, tb, ry, w_sem, send, recv):
    me_ep, me_tp = lax.axis_index("ep"), lax.axis_index("tp")
    near = me_ep + 1 - 2 * lax.rem(me_ep, 2)
    far = lax.rem(me_ep + 2, 4)
    peer = 1 - me_tp
    barrier = pltpu.get_barrier_semaphore()
    for dev in ({"ep": near}, {"ep": far}, {"tp": peer}):
        pl.semaphore_signal(barrier, inc=1, device_id=dev, device_id_type=pl.DeviceIdType.MESH)
    loads = [pltpu.make_async_copy(h, v, w_sem.at[m]) for m, (h, v) in enumerate(((wg_hbm, wg), (wu_hbm, wu), (wd_hbm, wd)))]
    for one in loads:
        one.start()
    pl.semaphore_wait(barrier, 3)
    n_c = xb.shape[1]
    rows = xb.shape[2]
    n_e = wg.shape[0]

    def move(kind, c):
        span = pl.ds(c * rows, rows)
        src, dst, dev = {
            PART: (part_ref.at[span], other.at[span], {"tp": peer}),
            NEAR: (xb.at[0, c], xb.at[1, c], {"ep": near}),
            FAR: (xb.at[0, c], xb.at[2, c], {"ep": far}),
            PASS: (xb.at[2, c], xb.at[3, c], {"ep": near}),
            BACK1: (ob.at[1, c], rb.at[0, c], {"ep": near}),
            BACK3: (ob.at[3, c], rb.at[1, c], {"ep": near}),
            BACKX: (fb.at[c], rf.at[c], {"ep": far}),
            BACKY: (tb.at[c], ry.at[c], {"tp": peer}),
        }[kind]
        return pltpu.make_async_remote_copy(src_ref=src, dst_ref=dst, send_sem=send.at[kind, c], recv_sem=recv.at[kind, c], device_id=dev, device_id_type=pl.DeviceIdType.MESH)

    def go(kind, c):
        move(kind, c).start()

    def arrive(kind, c):
        move(kind, c).wait_recv()

    def mid(c):
        arrive(PART, c)
        span = slice(c * rows, (c + 1) * rows)
        attn = part_ref[span, :].astype(F32) + other[span, :].astype(F32)
        row = (hid_ref[span, :].astype(F32) + attn + wide(bo_ref)).astype(BF)
        x1[span, :] = row
        h2 = norm_rows(row.astype(F32), wide(s2_ref), wide(b2_ref))
        xb[0, c, :, :1024] = h2
        logit = lax.dot_general(wr_ref[...], h2, (((1,), (1,)), ((), ())), preferred_element_type=F32)
        eid = lax.broadcasted_iota(jnp.int32, (32, rows), 0)
        picked = eid == ids_ref[0:1, span]
        for m in range(1, 8):
            picked = picked | (eid == ids_ref[m:m + 1, span])
        logit = jnp.where(picked, logit, -jnp.inf)
        ex = jnp.exp(logit - jnp.max(logit, axis=0, keepdims=True))
        prob = ex / jnp.sum(ex, axis=0, keepdims=True)
        full = jnp.concatenate([prob, jnp.zeros((96, rows), F32)], axis=0)
        xb[0, c, :, 1024:] = jnp.transpose(full).astype(BF)
        go(FAR, c)
        go(NEAR, c)

    def hand_on(c):
        arrive(FAR, c)
        go(PASS, c)

    def ready(c):
        arrive(NEAR, c)
        arrive(PASS, c)

    def give_back(c):
        go(BACK3, c)
        go(BACK1, c)

    def far_sum(c):
        arrive(BACK3, c)
        fb[c] = (ob[2, c].astype(F32) + rb[1, c].astype(F32)).astype(BF)
        go(BACKX, c)

    def all_sum(c):
        arrive(BACK1, c)
        arrive(BACKX, c)
        tb[c] = (ob[0, c].astype(F32) + rb[0, c].astype(F32) + rf[c].astype(F32)).astype(BF)
        go(BACKY, c)

    def last_sum(c):
        arrive(BACKY, c)
        span = slice(c * rows, (c + 1) * rows)
        moe = tb[c].astype(F32) + ry[c].astype(F32)
        out_ref[span, :] = (x1[span, :].astype(F32) + moe).astype(BF)

    for c in range(n_c):
        go(PART, c)
    mid(0)
    mid(1)
    hand_on(0)
    for one in loads:
        one.wait()
    table = {
        0: [(ready, 0)], 1: [(mid, 2)], 3: [(hand_on, 1)],
        4: [(give_back, 0), (ready, 1)], 5: [(mid, 3)], 6: [(far_sum, 0)], 7: [(hand_on, 2)],
        8: [(give_back, 1), (ready, 2)], 10: [(far_sum, 1)], 11: [(hand_on, 3)],
        12: [(give_back, 2), (ready, 3)], 13: [(all_sum, 0)], 14: [(far_sum, 2)],
    }
    parts = 4
    lane = lax.broadcasted_iota(jnp.int32, (4 * rows, 128), 1)

    def step(s, carry):
        for k, acts in table.items():
            @pl.when(s == k)
            def _():
                for act, c in acts:
                    act(c)
        c, q = s // parts, lax.rem(s, parts)

        @pl.when(q == 0)
        def _():
            acc[...] = jnp.zeros_like(acc)

        x = jnp.concatenate([xb[n, c, :, :1024] for n in range(4)], axis=0)
        gates = jnp.concatenate([xb[n, c, :, 1024:] for n in range(4)], axis=0).astype(F32)
        total = None
        for m in range(n_e // parts):
            e = q * (n_e // parts) + m
            gate = jnp.dot(x, wg[e], preferred_element_type=F32)
            up = jnp.dot(x, wu[e], preferred_element_type=F32)
            act = (gate * jax.nn.sigmoid(gate) * up).astype(BF)
            y = jnp.dot(act, wd[e], preferred_element_type=F32)
            g_one = jnp.sum(jnp.where(lane == me_ep * n_e + e, gates, 0.0), axis=-1, keepdims=True)
            acc[...] += g_one * y

        @pl.when(q == parts - 1)
        def _():
            for n in range(4):
                ob[n, c] = acc[n * rows:(n + 1) * rows, :].astype(BF)
        return carry

    lax.fori_loop(0, n_c * parts, step, 0)
    give_back(3)
    all_sum(1)
    far_sum(3)
    all_sum(2)
    last_sum(0)
    last_sum(1)
    all_sum(3)
    last_sum(2)
    last_sum(3)
    for kind in range(8):
        for c in range(n_c):
            move(kind, c).wait_send()


def moe_layer(hidden, part, b_out, s2, b2, wr_t, ids, wg, wu, wd):
    n_batch = hidden.shape[0]
    rows = n_batch // CHUNKS
    vmem = pl.BlockSpec(memory_space=pltpu.VMEM)
    hbm = pl.BlockSpec(memory_space=pl.ANY)
    blocks = lambda *lead: pltpu.VMEM(lead + (CHUNKS, rows, 1024), BF)
    return pl.pallas_call(
        moe_kernel,
        in_specs=[vmem] * 7 + [hbm] * 3, out_specs=vmem,
        out_shape=jax.ShapeDtypeStruct((n_batch, 1024), BF),
        scratch_shapes=[
            pltpu.VMEM((n_batch, 1024), BF), pltpu.VMEM((n_batch, 1024), BF), pltpu.VMEM((4, CHUNKS, rows, WIDE), BF),
            pltpu.VMEM(wg.shape, BF), pltpu.VMEM(wu.shape, BF), pltpu.VMEM(wd.shape, BF),
            pltpu.VMEM((4 * rows, 1024), F32), blocks(4), blocks(2), blocks(), blocks(), blocks(), blocks(),
            pltpu.SemaphoreType.DMA((3,)), pltpu.SemaphoreType.DMA((8, CHUNKS)), pltpu.SemaphoreType.DMA((8, CHUNKS))],
        compiler_params=pltpu.CompilerParams(collective_id=0, has_side_effects=True, vmem_limit_bytes=VMEM_LIMIT),
        cost_estimate=pl.CostEstimate(flops=26_000_000_000, bytes_accessed=14_000_000, transcendentals=0),
        name="moe",
    )(part, hidden, b_out, s2, b2, wr_t, ids, wg, wu, wd)


def solution(mesh):
    token_rows = P(('dp', 'ep'), None)
    token_vec = P(('dp', 'ep'))
    cache_spec = P(('dp', 'ep'), None, 'tp', None)
    expert_in = P('ep', None, 'tp')
    expert_down = P('ep', 'tp', None)

    def device_step(hidden, seq_lens, rope_cos, rope_sin, ln1_scale, ln1_bias, w_qkv, b_qkv, w_out, b_out, k_cache, v_cache, ln2_scale, ln2_bias, w_router, expert_ids, w_gate, w_up, w_down):
        n_batch = hidden.shape[0]
        kt, vt = (jnp.transpose(c, (0, 2, 3, 1)) for c in (k_cache, v_cache))
        part, *caches = attention(0, n_batch, seq_lens, hidden, rope_cos.T, rope_sin.T, ln1_scale, ln1_bias, w_qkv, b_qkv, w_out, kt, vt, None)
        out = moe_layer(hidden, part, b_out, ln2_scale, ln2_bias, w_router.T, expert_ids.T, w_gate, w_up, w_down)
        return out, *(jnp.transpose(c, (0, 3, 1, 2)) for c in caches)

    in_specs = (token_rows, token_vec, token_rows, token_rows, P(), P(), P(None, 'tp'), P('tp'), P('tp', None), P(), cache_spec, cache_spec, P(), P(), P(), token_rows, expert_in, expert_in, expert_down)
    step = jax.shard_map(device_step, mesh=mesh, in_specs=in_specs, out_specs=(token_rows, cache_spec, cache_spec), check_vma=False)
    return step
```

```python
import functools

import jax
import jax.numpy as jnp
from jax import lax
from jax.experimental import pallas as pl
from jax.experimental.pallas import tpu as pltpu
from jax.sharding import PartitionSpec as P

EPS = 1e-5
BF = jnp.bfloat16
F32 = jnp.float32
CHUNKS = 4
SUB = 128
BB = 16
GROUP = 4
WIDE = 1024 + 128
SLOTS = 8
AHEAD = 5
VMEM_LIMIT = 60 * 1024 * 1024


def norm_rows(x, scale, bias):
    mean = jnp.mean(x, axis=-1, keepdims=True)
    cen = x - mean
    var = jnp.mean(cen * cen, axis=-1, keepdims=True)
    return (cen * lax.rsqrt(var + EPS) * scale + bias).astype(BF)


def wide(ref):
    return ref[...].astype(F32).reshape(1, -1)


def attention_kernel(base_row, has_prev, len_ref, hid_ref, cos_ref, sin_ref, s1_ref, b1_ref, bqkv_ref, wqkv_hbm, wout_hbm, k_hbm, v_hbm, *rest):
    part_ref, ko_hbm, vo_hbm = rest[2 * has_prev:2 * has_prev + 3]
    wqkv_ref, wout_ref, kb_ref, vb_ref, qs_ref, kt_ref, vt_ref, sc_ref, pr_ref, cx_ref, ctx_ref, kc_ref, vc_ref, in_sem, out_sem, w_sem = rest[2 * has_prev + 3:]
    step = pl.program_id(0)
    n_step = pl.num_programs(0)
    per_sub = SUB // BB
    j = lax.rem(step, per_sub)
    lane = lax.broadcasted_iota(jnp.int32, (SUB, 128), 1)
    low = lane < 64

    def moves(s, out):
        slot = lax.rem(s, SLOTS)
        src = pl.ds(base_row + s * BB, BB)
        pairs = ((k_hbm, kb_ref, ko_hbm, 0), (v_hbm, vb_ref, vo_hbm, 1))
        if out:
            return [(pltpu.make_async_copy(buf.at[slot], dst.at[src], out_sem.at[t, slot]), t) for _, buf, dst, t in pairs]
        return [(pltpu.make_async_copy(hbm.at[src], buf.at[slot], in_sem.at[t, slot]), t) for hbm, buf, _, t in pairs]

    def begin(s, out):
        for copy, t in moves(s, out):
            copy.start(priority=t)

    def finish(s, out):
        for copy, _ in moves(s, out):
            copy.wait()

    load_qkv = pltpu.make_async_copy(wqkv_hbm, wqkv_ref, w_sem.at[0])
    load_out = pltpu.make_async_copy(wout_hbm, wout_ref, w_sem.at[1])

    @pl.when(step == 0)
    def _():
        load_qkv.start()
        for s in range(AHEAD):
            begin(s, False)
        load_out.start()
        load_qkv.wait()

    @pl.when(j == 0)
    def _():
        normed = norm_rows(hid_ref[...].astype(F32), wide(s1_ref), wide(b1_ref))
        qkv = jnp.dot(normed, wqkv_ref[...], preferred_element_type=F32) + wide(bqkv_ref)
        qkv = qkv.astype(BF).astype(F32)
        col = [qkv[:, m * 128:(m + 1) * 128] for m in range(8)]
        rol = [pltpu.roll(c, 64, 1) for c in col]

        def first(a, b):
            return jnp.where(low, col[a], rol[b])

        def second(a, b):
            return jnp.where(low, rol[a], col[b])

        cos_t, sin_t = cos_ref[...], sin_ref[...]
        cos = jnp.transpose(jnp.concatenate([cos_t] * 4, axis=0))
        sin = jnp.transpose(jnp.concatenate([-sin_t, sin_t] * 2, axis=0))

        def rope(x):
            other = jnp.where(lane % 64 < 32, pltpu.roll(x, 96, 1), pltpu.roll(x, 32, 1))
            return (x * cos + other * sin).astype(BF).astype(F32)

        for h in range(2):
            q0 = rope(first(4 * h, 4 * h + 2))
            q1 = rope(second(4 * h, 4 * h + 2))
            kk = rope(first(4 * h + 1, 4 * h + 3))
            vv = second(4 * h + 1, 4 * h + 3)
            kt_ref[h * 128:(h + 1) * 128, :] = jnp.transpose(kk)
            vt_ref[h * 128:(h + 1) * 128, :] = jnp.transpose(vv)
            for r in range(8):
                src = q0 if r % 2 == 0 else q1
                if r // 4 == h:
                    src = jnp.where(low if (r // 2) % 2 == 0 else ~low, src, 0.0)
                else:
                    src = jnp.zeros_like(src)
                qs_ref[pl.ds(h * SUB * 8 + r, SUB, stride=8), :] = src

    slot = lax.rem(step, SLOTS)
    finish(step, False)
    lane8 = lax.broadcasted_iota(jnp.int32, (8, 128), 1)
    lane256 = lax.broadcasted_iota(jnp.int32, (256, 128), 1)
    row0 = pl.multiple_of(j * BB * 8, BB * 8)
    base = base_row + step * BB
    pos = [len_ref[base + b] for b in range(BB)]
    slow = []

    def fetch(source, b):
        for new, ref in ((kc_ref, kt_ref), (vc_ref, vt_ref)):
            for r in range(0, 256, 8):
                new[b, r:r + 8, :] = jnp.take_along_axis(ref[r:r + 8, :], source, axis=1, mode="promise_in_bounds")

    for t in range(0, BB, GROUP):
        source = jnp.zeros((8, 128), jnp.int32)
        same = None
        for m in range(t, t + GROUP):
            source = jnp.where(lane8 == pos[m], j * BB + m, source)
            for n in range(t, m):
                hit = pos[m] == pos[n]
                same = hit if same is None else same | hit
        fetch(source, t)
        slow.append(same)

        @pl.when(same)
        def _():
            for m in range(t, t + GROUP):
                fetch(jnp.full((8, 128), j * BB + m, jnp.int32), m)

    def placed(buf, cols, b):
        t = b // GROUP * GROUP
        mine = t if b == t else jnp.where(slow[b // GROUP], b, t)
        old = buf[slot, b].reshape(256, 128).astype(F32)
        new = jnp.where(lane256 == pos[b], cols[mine], old).astype(BF)
        buf[slot, b] = new.reshape(4, 64, 128)
        return new

    for b in range(BB):
        k_new = placed(kb_ref, kc_ref, b)
        q_one = jnp.concatenate([qs_ref[pl.ds(row0 + h * SUB * 8 + b * 8, 8), :] for h in range(2)], axis=1).astype(BF)
        s_one = jnp.dot(q_one, k_new, preferred_element_type=F32) * 0.125
        sc_ref[b * 8:(b + 1) * 8, :] = jnp.where(lane8 <= pos[b], s_one, -jnp.inf)
    s_all = sc_ref[...]
    e_all = jnp.exp(s_all - jnp.max(s_all, axis=-1, keepdims=True))
    pr_ref[...] = e_all / jnp.sum(e_all, axis=-1, keepdims=True)
    for b in range(BB):
        v_new = placed(vb_ref, vc_ref, b)
        p_one = pr_ref[b * 8:(b + 1) * 8, :].astype(BF)
        c_one = lax.dot_general(p_one, v_new, (((1,), (1,)), ((), ())), preferred_element_type=F32)
        cx_ref[b * 8:(b + 1) * 8, :] = c_one[:, :128]
        cx_ref[BB * 8 + b * 8:BB * 8 + (b + 1) * 8, :] = c_one[:, 128:]
    low_b = lax.broadcasted_iota(jnp.int32, (BB, 128), 1) < 64
    for h in range(2):
        for g in range(2):
            r = 4 * h + 2 * g
            one = cx_ref[pl.ds(h * BB * 8 + r, BB, stride=8), :]
            two = cx_ref[pl.ds(h * BB * 8 + r + 1, BB, stride=8), :]
            if g == 0:
                both = jnp.where(low_b, one, pltpu.roll(two, 64, 1))
            else:
                both = jnp.where(low_b, pltpu.roll(one, 64, 1), two)
            ctx_ref[pl.ds(pl.multiple_of(j * BB, BB), BB), (2 * h + g) * 128:(2 * h + g + 1) * 128] = both.astype(BF)

    begin(step, True)

    @pl.when(step + AHEAD < n_step)
    def _():
        @pl.when(step + AHEAD >= SLOTS)
        def _():
            finish(step + AHEAD - SLOTS, True)
        begin(step + AHEAD, False)

    @pl.when(step == per_sub - 1)
    def _():
        load_out.wait()

    @pl.when(j == per_sub - 1)
    def _():
        part_ref[...] = jnp.dot(ctx_ref[...], wout_ref[...], preferred_element_type=F32).astype(BF)

    @pl.when(step == n_step - 1)
    def _():
        for back in range(SLOTS - 1, -1, -1):
            @pl.when(step >= back)
            def _():
                finish(step - back, True)


def attention(chunk, rows, lens, hidden, cos_t, sin_t, s1, b1, wqkv, bqkv, wout, kt, vt, prev):
    per_sub = SUB // BB
    n_step = rows // BB
    first = chunk * rows // SUB
    vec = pl.BlockSpec((1024,), lambda i, s: (0,))
    hbm = pl.BlockSpec(memory_space=pl.ANY)
    in_specs = [
        pl.BlockSpec((SUB, 1024), lambda i, s: (first + i // per_sub, 0)),
        pl.BlockSpec((32, SUB), lambda i, s: (0, first + i // per_sub)),
        pl.BlockSpec((32, SUB), lambda i, s: (0, first + i // per_sub)),
        vec, vec, vec, hbm, hbm, hbm, hbm,
    ]
    args = [lens, hidden, cos_t, sin_t, s1, b1, bqkv, wqkv, wout, kt, vt]
    aliases = {}
    if prev is not None:
        in_specs += [hbm, hbm]
        aliases = {len(args): 1, len(args) + 1: 2}
        args += list(prev)
    return pl.pallas_call(
        functools.partial(attention_kernel, chunk * rows, int(prev is not None)),
        grid_spec=pltpu.PrefetchScalarGridSpec(
            num_scalar_prefetch=1, grid=(n_step,), in_specs=in_specs,
            out_specs=[pl.BlockSpec((SUB, 1024), lambda i, s: (i // per_sub, 0)), hbm, hbm],
            scratch_shapes=[
                pltpu.VMEM(wqkv.shape, BF), pltpu.VMEM(wout.shape, BF),
                pltpu.VMEM((SLOTS, BB, 4, 64, 128), BF), pltpu.VMEM((SLOTS, BB, 4, 64, 128), BF),
                pltpu.VMEM((2 * SUB * 8, 128), F32), pltpu.VMEM((256, SUB), F32), pltpu.VMEM((256, SUB), F32),
                pltpu.VMEM((BB * 8, 128), F32), pltpu.VMEM((BB * 8, 128), F32),
                pltpu.VMEM((2 * BB * 8, 128), F32), pltpu.VMEM((SUB, 512), BF),
                pltpu.VMEM((BB, 256, 128), F32), pltpu.VMEM((BB, 256, 128), F32),
                pltpu.SemaphoreType.DMA((2, SLOTS)), pltpu.SemaphoreType.DMA((2, SLOTS)), pltpu.SemaphoreType.DMA((2,))]),
        out_shape=[jax.ShapeDtypeStruct((rows, 1024), BF), jax.ShapeDtypeStruct(kt.shape, BF), jax.ShapeDtypeStruct(vt.shape, BF)],
        input_output_aliases=aliases,
        compiler_params=pltpu.CompilerParams(dimension_semantics=("arbitrary",), vmem_limit_bytes=VMEM_LIMIT),
        cost_estimate=pl.CostEstimate(flops=rows * 20_000_000, bytes_accessed=rows * 262144, transcendentals=0),
        name="attention",
    )(*args)


PART, NEAR, FAR, PASS, BACK1, BACK3, BACKX, BACKY = range(8)


def moe_kernel(part_ref, hid_ref, bo_ref, s2_ref, b2_ref, wr_ref, ids_ref, wg_hbm, wu_hbm, wd_hbm, out_ref,
               other, x1, xb, wg, wu, wd, acc, ob, rb, fb, rf, tb, ry, w_sem, send, recv):
    me_ep, me_tp = lax.axis_index("ep"), lax.axis_index("tp")
    near = me_ep + 1 - 2 * lax.rem(me_ep, 2)
    far = lax.rem(me_ep + 2, 4)
    peer = 1 - me_tp
    barrier = pltpu.get_barrier_semaphore()
    for dev in ({"ep": near}, {"ep": far}, {"tp": peer}):
        pl.semaphore_signal(barrier, inc=1, device_id=dev, device_id_type=pl.DeviceIdType.MESH)
    loads = [pltpu.make_async_copy(h, v, w_sem.at[m]) for m, (h, v) in enumerate(((wg_hbm, wg), (wu_hbm, wu), (wd_hbm, wd)))]
    for one in loads:
        one.start()
    pl.semaphore_wait(barrier, 3)
    n_c = xb.shape[1]
    rows = xb.shape[2]
    n_e = wg.shape[0]

    def move(kind, c):
        span = pl.ds(c * rows, rows)
        src, dst, dev = {
            PART: (part_ref.at[span], other.at[span], {"tp": peer}),
            NEAR: (xb.at[0, c], xb.at[1, c], {"ep": near}),
            FAR: (xb.at[0, c], xb.at[2, c], {"ep": far}),
            PASS: (xb.at[2, c], xb.at[3, c], {"ep": near}),
            BACK1: (ob.at[1, c], rb.at[0, c], {"ep": near}),
            BACK3: (ob.at[3, c], rb.at[1, c], {"ep": near}),
            BACKX: (fb.at[c], rf.at[c], {"ep": far}),
            BACKY: (tb.at[c], ry.at[c], {"tp": peer}),
        }[kind]
        return pltpu.make_async_remote_copy(src_ref=src, dst_ref=dst, send_sem=send.at[kind, c], recv_sem=recv.at[kind, c], device_id=dev, device_id_type=pl.DeviceIdType.MESH)

    def go(kind, c):
        move(kind, c).start()

    def arrive(kind, c):
        move(kind, c).wait_recv()

    def mid(c):
        arrive(PART, c)
        span = slice(c * rows, (c + 1) * rows)
        attn = part_ref[span, :].astype(F32) + other[span, :].astype(F32)
        row = (hid_ref[span, :].astype(F32) + attn + wide(bo_ref)).astype(BF)
        x1[span, :] = row
        h2 = norm_rows(row.astype(F32), wide(s2_ref), wide(b2_ref))
        xb[0, c, :, :1024] = h2
        logit = lax.dot_general(wr_ref[...], h2, (((1,), (1,)), ((), ())), preferred_element_type=F32)
        eid = lax.broadcasted_iota(jnp.int32, (32, rows), 0)
        picked = eid == ids_ref[0:1, span]
        for m in range(1, 8):
            picked = picked | (eid == ids_ref[m:m + 1, span])
        logit = jnp.where(picked, logit, -jnp.inf)
        ex = jnp.exp(logit - jnp.max(logit, axis=0, keepdims=True))
        prob = ex / jnp.sum(ex, axis=0, keepdims=True)
        full = jnp.concatenate([prob, jnp.zeros((96, rows), F32)], axis=0)
        xb[0, c, :, 1024:] = jnp.transpose(full).astype(BF)
        go(FAR, c)
        go(NEAR, c)

    def hand_on(c):
        arrive(FAR, c)
        go(PASS, c)

    def ready(c):
        arrive(NEAR, c)
        arrive(PASS, c)

    def give_back(c):
        go(BACK3, c)
        go(BACK1, c)

    def far_sum(c):
        arrive(BACK3, c)
        fb[c] = (ob[2, c].astype(F32) + rb[1, c].astype(F32)).astype(BF)
        go(BACKX, c)

    def all_sum(c):
        arrive(BACK1, c)
        arrive(BACKX, c)
        tb[c] = (ob[0, c].astype(F32) + rb[0, c].astype(F32) + rf[c].astype(F32)).astype(BF)
        go(BACKY, c)

    def last_sum(c):
        arrive(BACKY, c)
        span = slice(c * rows, (c + 1) * rows)
        moe = tb[c].astype(F32) + ry[c].astype(F32)
        out_ref[span, :] = (x1[span, :].astype(F32) + moe).astype(BF)

    for c in range(n_c):
        go(PART, c)
    mid(0)
    mid(1)
    hand_on(0)
    for one in loads:
        one.wait()
    table = {
        0: [(ready, 0)], 1: [(mid, 2)], 3: [(hand_on, 1)],
        4: [(give_back, 0), (ready, 1)], 5: [(mid, 3)], 6: [(far_sum, 0)], 7: [(hand_on, 2)],
        8: [(give_back, 1), (ready, 2)], 10: [(far_sum, 1)], 11: [(hand_on, 3)],
        12: [(give_back, 2), (ready, 3)], 13: [(all_sum, 0)], 14: [(far_sum, 2)],
    }
    parts = 4
    lane = lax.broadcasted_iota(jnp.int32, (4 * rows, 128), 1)

    def step(s, carry):
        for k, acts in table.items():
            @pl.when(s == k)
            def _():
                for act, c in acts:
                    act(c)
        c, q = s // parts, lax.rem(s, parts)

        @pl.when(q == 0)
        def _():
            acc[...] = jnp.zeros_like(acc)

        x = jnp.concatenate([xb[n, c, :, :1024] for n in range(4)], axis=0)
        gates = jnp.concatenate([xb[n, c, :, 1024:] for n in range(4)], axis=0).astype(F32)
        total = None
        for m in range(n_e // parts):
            e = q * (n_e // parts) + m
            gate = jnp.dot(x, wg[e], preferred_element_type=F32)
            up = jnp.dot(x, wu[e], preferred_element_type=F32)
            act = (gate * jax.nn.sigmoid(gate) * up).astype(BF)
            y = jnp.dot(act, wd[e], preferred_element_type=F32)
            g_one = jnp.sum(jnp.where(lane == me_ep * n_e + e, gates, 0.0), axis=-1, keepdims=True)
            acc[...] += g_one * y

        @pl.when(q == parts - 1)
        def _():
            for n in range(4):
                ob[n, c] = acc[n * rows:(n + 1) * rows, :].astype(BF)
        return carry

    lax.fori_loop(0, n_c * parts, step, 0)
    give_back(3)
    all_sum(1)
    far_sum(3)
    all_sum(2)
    last_sum(0)
    last_sum(1)
    all_sum(3)
    last_sum(2)
    last_sum(3)
    for kind in range(8):
        for c in range(n_c):
            move(kind, c).wait_send()


def moe_layer(hidden, part, b_out, s2, b2, wr_t, ids, wg, wu, wd):
    n_batch = hidden.shape[0]
    rows = n_batch // CHUNKS
    vmem = pl.BlockSpec(memory_space=pltpu.VMEM)
    hbm = pl.BlockSpec(memory_space=pl.ANY)
    blocks = lambda *lead: pltpu.VMEM(lead + (CHUNKS, rows, 1024), BF)
    return pl.pallas_call(
        moe_kernel,
        in_specs=[vmem] * 7 + [hbm] * 3, out_specs=vmem,
        out_shape=jax.ShapeDtypeStruct((n_batch, 1024), BF),
        scratch_shapes=[
            pltpu.VMEM((n_batch, 1024), BF), pltpu.VMEM((n_batch, 1024), BF), pltpu.VMEM((4, CHUNKS, rows, WIDE), BF),
            pltpu.VMEM(wg.shape, BF), pltpu.VMEM(wu.shape, BF), pltpu.VMEM(wd.shape, BF),
            pltpu.VMEM((4 * rows, 1024), F32), blocks(4), blocks(2), blocks(), blocks(), blocks(), blocks(),
            pltpu.SemaphoreType.DMA((3,)), pltpu.SemaphoreType.DMA((8, CHUNKS)), pltpu.SemaphoreType.DMA((8, CHUNKS))],
        compiler_params=pltpu.CompilerParams(collective_id=0, has_side_effects=True, vmem_limit_bytes=VMEM_LIMIT),
        cost_estimate=pl.CostEstimate(flops=26_000_000_000, bytes_accessed=14_000_000, transcendentals=0),
        name="moe",
    )(part, hidden, b_out, s2, b2, wr_t, ids, wg, wu, wd)


def solution(mesh):
    token_rows = P(('dp', 'ep'), None)
    token_vec = P(('dp', 'ep'))
    cache_spec = P(('dp', 'ep'), None, 'tp', None)
    expert_in = P('ep', None, 'tp')
    expert_down = P('ep', 'tp', None)

    def device_step(hidden, seq_lens, rope_cos, rope_sin, ln1_scale, ln1_bias, w_qkv, b_qkv, w_out, b_out, k_cache, v_cache, ln2_scale, ln2_bias, w_router, expert_ids, w_gate, w_up, w_down):
        n_batch = hidden.shape[0]
        kt, vt = (jnp.transpose(c, (0, 2, 3, 1)) for c in (k_cache, v_cache))
        part, *caches = attention(0, n_batch, seq_lens, hidden, rope_cos.T, rope_sin.T, ln1_scale, ln1_bias, w_qkv, b_qkv, w_out, kt, vt, None)
        out = moe_layer(hidden, part, b_out, ln2_scale, ln2_bias, w_router.T, expert_ids.T, w_gate, w_up, w_down)
        return out, *(jnp.transpose(c, (0, 3, 1, 2)) for c in caches)

    in_specs = (token_rows, token_vec, token_rows, token_rows, P(), P(), P(None, 'tp'), P('tp'), P('tp', None), P(), cache_spec, cache_spec, P(), P(), P(), token_rows, expert_in, expert_in, expert_down)
    step = jax.shard_map(device_step, mesh=mesh, in_specs=in_specs, out_specs=(token_rows, cache_spec, cache_spec), check_vma=False)
    return step
```

```python
import functools

import jax
import jax.numpy as jnp
from jax import lax
from jax.experimental import pallas as pl
from jax.experimental.pallas import tpu as pltpu
from jax.sharding import PartitionSpec as P

EPS = 1e-5
BF = jnp.bfloat16
F32 = jnp.float32
CHUNKS = 4
HEAD = 2
TAIL = 4
SUB = 128
BB = 16
WIDE = 1024 + 128
SLOTS = 8
AHEAD = 5
VMEM_LIMIT = 60 * 1024 * 1024


def norm_rows(x, scale, bias):
    mean = jnp.mean(x, axis=-1, keepdims=True)
    cen = x - mean
    var = jnp.mean(cen * cen, axis=-1, keepdims=True)
    return (cen * lax.rsqrt(var + EPS) * scale + bias).astype(BF)


def wide(ref):
    return ref[...].astype(F32).reshape(1, -1)


def attention_kernel(base_row, has_prev, len_ref, hid_ref, cos_ref, sin_ref, s1_ref, b1_ref, bqkv_ref, wqkv_hbm, wout_hbm, k_hbm, v_hbm, *rest):
    part_ref, ko_hbm, vo_hbm = rest[2 * has_prev:2 * has_prev + 3]
    wqkv_ref, wout_ref, kb_ref, vb_ref, qs_ref, kt_ref, vt_ref, sc_ref, pr_ref, cx_ref, ctx_ref, in_sem, out_sem, w_sem = rest[2 * has_prev + 3:]
    step = pl.program_id(0)
    n_step = pl.num_programs(0)
    per_sub = SUB // BB
    j = lax.rem(step, per_sub)
    lane = lax.broadcasted_iota(jnp.int32, (SUB, 128), 1)
    low = lane < 64

    def moves(s, out):
        slot = lax.rem(s, SLOTS)
        src = pl.ds(base_row + s * BB, BB)
        pairs = ((k_hbm, kb_ref, ko_hbm, 0), (v_hbm, vb_ref, vo_hbm, 1))
        if out:
            return [(pltpu.make_async_copy(buf.at[slot], dst.at[src], out_sem.at[t, slot]), t) for _, buf, dst, t in pairs]
        return [(pltpu.make_async_copy(hbm.at[src], buf.at[slot], in_sem.at[t, slot]), t) for hbm, buf, _, t in pairs]

    def begin(s, out):
        for copy, t in moves(s, out):
            copy.start(priority=t)

    def finish(s, out):
        for copy, _ in moves(s, out):
            copy.wait()

    load_qkv = pltpu.make_async_copy(wqkv_hbm, wqkv_ref, w_sem.at[0])
    load_out = pltpu.make_async_copy(wout_hbm, wout_ref, w_sem.at[1])

    @pl.when(step == 0)
    def _():
        load_qkv.start()
        for s in range(AHEAD):
            begin(s, False)
        load_out.start()
        load_qkv.wait()

    @pl.when(j == 0)
    def _():
        normed = norm_rows(hid_ref[...].astype(F32), wide(s1_ref), wide(b1_ref))
        qkv = jnp.dot(normed, wqkv_ref[...], preferred_element_type=F32) + wide(bqkv_ref)
        qkv = qkv.astype(BF).astype(F32)
        col = [qkv[:, m * 128:(m + 1) * 128] for m in range(8)]
        rol = [pltpu.roll(c, 64, 1) for c in col]

        def first(a, b):
            return jnp.where(low, col[a], rol[b])

        def second(a, b):
            return jnp.where(low, rol[a], col[b])

        cos_t, sin_t = cos_ref[...], sin_ref[...]
        cos = jnp.transpose(jnp.concatenate([cos_t] * 4, axis=0))
        sin = jnp.transpose(jnp.concatenate([-sin_t, sin_t] * 2, axis=0))

        def rope(x):
            other = jnp.where(lane % 64 < 32, pltpu.roll(x, 96, 1), pltpu.roll(x, 32, 1))
            return (x * cos + other * sin).astype(BF).astype(F32)

        for h in range(2):
            q0 = rope(first(4 * h, 4 * h + 2))
            q1 = rope(second(4 * h, 4 * h + 2))
            kk = rope(first(4 * h + 1, 4 * h + 3))
            vv = second(4 * h + 1, 4 * h + 3)
            kt_ref[h * 128:(h + 1) * 128, :] = jnp.transpose(kk)
            vt_ref[h * 128:(h + 1) * 128, :] = jnp.transpose(vv)
            for r in range(8):
                src = q0 if r % 2 == 0 else q1
                if r // 4 == h:
                    src = jnp.where(low if (r // 2) % 2 == 0 else ~low, src, 0.0)
                else:
                    src = jnp.zeros_like(src)
                qs_ref[pl.ds(h * SUB * 8 + r, SUB, stride=8), :] = src

    slot = lax.rem(step, SLOTS)
    finish(step, False)
    shift = lax.rem(SUB - j * BB, SUB)
    kt = pltpu.roll(kt_ref[...], shift, 1)
    vt = pltpu.roll(vt_ref[...], shift, 1)[:, :BB].astype(BF)
    unit_row = lax.broadcasted_iota(jnp.int32, (BB, 256), 0)
    unit_col = lax.broadcasted_iota(jnp.int32, (BB, 256), 1) // 128
    lane8 = lax.broadcasted_iota(jnp.int32, (8, 128), 1)
    lane256 = lax.broadcasted_iota(jnp.int32, (256, 128), 1)
    row0 = pl.multiple_of(j * BB * 8, BB * 8)
    base = base_row + step * BB

    def placed(buf, cols, b):
        pos = len_ref[base + b]
        old = buf[slot, b].reshape(256, 128).astype(F32)
        new = jnp.where(lane256 == pos, cols, old).astype(BF)
        buf[slot, b] = new.reshape(4, 64, 128)
        return pos, new

    for b in range(BB):
        pos, k_new = placed(kb_ref, kt[:, b:b + 1], b)
        q_one = jnp.concatenate([qs_ref[pl.ds(row0 + h * SUB * 8 + b * 8, 8), :] for h in range(2)], axis=1).astype(BF)
        s_one = jnp.dot(q_one, k_new, preferred_element_type=F32) * 0.125
        sc_ref[b * 8:(b + 1) * 8, :] = jnp.where(lane8 <= pos, s_one, -jnp.inf)
    s_all = sc_ref[...]
    e_all = jnp.exp(s_all - jnp.max(s_all, axis=-1, keepdims=True))
    pr_ref[...] = e_all / jnp.sum(e_all, axis=-1, keepdims=True)
    for b in range(BB):
        if b % 2 == 0:
            unit = (unit_row == unit_col + b).astype(F32).astype(BF)
            two = jnp.dot(vt, unit, preferred_element_type=F32)
        _, v_new = placed(vb_ref, two[:, (b % 2) * 128:(b % 2 + 1) * 128], b)
        p_one = pr_ref[b * 8:(b + 1) * 8, :].astype(BF)
        c_one = lax.dot_general(p_one, v_new, (((1,), (1,)), ((), ())), preferred_element_type=F32)
        cx_ref[b * 8:(b + 1) * 8, :] = c_one[:, :128]
        cx_ref[BB * 8 + b * 8:BB * 8 + (b + 1) * 8, :] = c_one[:, 128:]
    low_b = lax.broadcasted_iota(jnp.int32, (BB, 128), 1) < 64
    for h in range(2):
        for g in range(2):
            r = 4 * h + 2 * g
            one = cx_ref[pl.ds(h * BB * 8 + r, BB, stride=8), :]
            two = cx_ref[pl.ds(h * BB * 8 + r + 1, BB, stride=8), :]
            if g == 0:
                both = jnp.where(low_b, one, pltpu.roll(two, 64, 1))
            else:
                both = jnp.where(low_b, pltpu.roll(one, 64, 1), two)
            ctx_ref[pl.ds(pl.multiple_of(j * BB, BB), BB), (2 * h + g) * 128:(2 * h + g + 1) * 128] = both.astype(BF)

    begin(step, True)

    @pl.when(step + AHEAD < n_step)
    def _():
        @pl.when(step + AHEAD >= SLOTS)
        def _():
            finish(step + AHEAD - SLOTS, True)
        begin(step + AHEAD, False)

    @pl.when(step == per_sub - 1)
    def _():
        load_out.wait()

    @pl.when(j == per_sub - 1)
    def _():
        part_ref[...] = jnp.dot(ctx_ref[...], wout_ref[...], preferred_element_type=F32).astype(BF)

    @pl.when(step == n_step - 1)
    def _():
        for back in range(SLOTS - 1, -1, -1):
            @pl.when(step >= back)
            def _():
                finish(step - back, True)


def attention(chunk, rows, lens, hidden, cos_t, sin_t, s1, b1, wqkv, bqkv, wout, kt, vt, prev):
    per_sub = SUB // BB
    n_step = rows // BB
    first = chunk * rows // SUB
    vec = pl.BlockSpec((1024,), lambda i, s: (0,))
    hbm = pl.BlockSpec(memory_space=pl.ANY)
    in_specs = [
        pl.BlockSpec((SUB, 1024), lambda i, s: (first + i // per_sub, 0)),
        pl.BlockSpec((32, SUB), lambda i, s: (0, first + i // per_sub)),
        pl.BlockSpec((32, SUB), lambda i, s: (0, first + i // per_sub)),
        vec, vec, vec, hbm, hbm, hbm, hbm,
    ]
    args = [lens, hidden, cos_t, sin_t, s1, b1, bqkv, wqkv, wout, kt, vt]
    aliases = {}
    if prev is not None:
        in_specs += [hbm, hbm]
        aliases = {len(args): 1, len(args) + 1: 2}
        args += list(prev)
    return pl.pallas_call(
        functools.partial(attention_kernel, chunk * rows, int(prev is not None)),
        grid_spec=pltpu.PrefetchScalarGridSpec(
            num_scalar_prefetch=1, grid=(n_step,), in_specs=in_specs,
            out_specs=[pl.BlockSpec((SUB, 1024), lambda i, s: (i // per_sub, 0)), hbm, hbm],
            scratch_shapes=[
                pltpu.VMEM(wqkv.shape, BF), pltpu.VMEM(wout.shape, BF),
                pltpu.VMEM((SLOTS, BB, 4, 64, 128), BF), pltpu.VMEM((SLOTS, BB, 4, 64, 128), BF),
                pltpu.VMEM((2 * SUB * 8, 128), F32), pltpu.VMEM((256, SUB), F32), pltpu.VMEM((256, SUB), F32),
                pltpu.VMEM((BB * 8, 128), F32), pltpu.VMEM((BB * 8, 128), F32),
                pltpu.VMEM((2 * BB * 8, 128), F32), pltpu.VMEM((SUB, 512), BF),
                pltpu.SemaphoreType.DMA((2, SLOTS)), pltpu.SemaphoreType.DMA((2, SLOTS)), pltpu.SemaphoreType.DMA((2,))]),
        out_shape=[jax.ShapeDtypeStruct((rows, 1024), BF), jax.ShapeDtypeStruct(kt.shape, BF), jax.ShapeDtypeStruct(vt.shape, BF)],
        input_output_aliases=aliases,
        compiler_params=pltpu.CompilerParams(dimension_semantics=("arbitrary",), vmem_limit_bytes=VMEM_LIMIT),
        cost_estimate=pl.CostEstimate(flops=rows * 20_000_000, bytes_accessed=rows * 262144, transcendentals=0),
        name="attention",
    )(*args)


PART, NEAR, FAR, PASS, BACK1, BACK3, BACKX, BACKY = range(8)


def moe_kernel(part_ref, hid_ref, bo_ref, s2_ref, b2_ref, wr_ref, ids_ref, wg_hbm, wu_hbm, wd_hbm, out_ref,
               other, x1, xb, wg, wu, wd, acc, ob, rb, fb, rf, tb, ry, w_sem, send, recv):
    me_ep, me_tp = lax.axis_index("ep"), lax.axis_index("tp")
    near = me_ep + 1 - 2 * lax.rem(me_ep, 2)
    far = lax.rem(me_ep + 2, 4)
    peer = 1 - me_tp
    barrier = pltpu.get_barrier_semaphore()
    for dev in ({"ep": near}, {"ep": far}, {"tp": peer}):
        pl.semaphore_signal(barrier, inc=1, device_id=dev, device_id_type=pl.DeviceIdType.MESH)
    loads = [pltpu.make_async_copy(h, v, w_sem.at[m]) for m, (h, v) in enumerate(((wg_hbm, wg), (wu_hbm, wu), (wd_hbm, wd)))]
    for one in loads:
        one.start()
    pl.semaphore_wait(barrier, 3)
    n_c = xb.shape[1]
    rows = xb.shape[2]
    n_e = wg.shape[0]

    split = {0: HEAD, n_c - 1: TAIL}

    def pieces(kind, c):
        early = kind in (PART, NEAR, FAR, PASS)
        count = split.get(c, 1) if (c == 0) == early else 1
        return [(c, p, count) for p in range(count)]

    def move(kind, c, p, count):
        size = rows // count
        sub = pl.ds(p * size, size)
        span = pl.ds(c * rows + p * size, size)
        src, dst, dev = {
            PART: (part_ref.at[span], other.at[span], {"tp": peer}),
            NEAR: (xb.at[0, c, sub], xb.at[1, c, sub], {"ep": near}),
            FAR: (xb.at[0, c, sub], xb.at[2, c, sub], {"ep": far}),
            PASS: (xb.at[2, c, sub], xb.at[3, c, sub], {"ep": near}),
            BACK1: (ob.at[1, c, sub], rb.at[0, c, sub], {"ep": near}),
            BACK3: (ob.at[3, c, sub], rb.at[1, c, sub], {"ep": near}),
            BACKX: (fb.at[c, sub], rf.at[c, sub], {"ep": far}),
            BACKY: (tb.at[c, sub], ry.at[c, sub], {"tp": peer}),
        }[kind]
        lane = p * n_c + c
        return pltpu.make_async_remote_copy(src_ref=src, dst_ref=dst, send_sem=send.at[kind, lane], recv_sem=recv.at[kind, lane], device_id=dev, device_id_type=pl.DeviceIdType.MESH)

    def go(kind, *at):
        move(kind, *at).start()

    def arrive(kind, *at):
        move(kind, *at).wait_recv()

    def rows_of(c, p, count):
        size = rows // count
        return slice(p * size, (p + 1) * size), slice(c * rows + p * size, c * rows + (p + 1) * size)

    def mid(c):
        for at in pieces(FAR, c):
            arrive(PART, *at)
            sub, span = rows_of(*at)
            attn = part_ref[span, :].astype(F32) + other[span, :].astype(F32)
            row = (hid_ref[span, :].astype(F32) + attn + wide(bo_ref)).astype(BF)
            x1[span, :] = row
            h2 = norm_rows(row.astype(F32), wide(s2_ref), wide(b2_ref))
            xb[0, c, sub, :1024] = h2
            size = h2.shape[0]
            logit = lax.dot_general(wr_ref[...], h2, (((1,), (1,)), ((), ())), preferred_element_type=F32)
            eid = lax.broadcasted_iota(jnp.int32, (32, size), 0)
            picked = eid == ids_ref[0:1, span]
            for m in range(1, 8):
                picked = picked | (eid == ids_ref[m:m + 1, span])
            logit = jnp.where(picked, logit, -jnp.inf)
            ex = jnp.exp(logit - jnp.max(logit, axis=0, keepdims=True))
            prob = ex / jnp.sum(ex, axis=0, keepdims=True)
            full = jnp.concatenate([prob, jnp.zeros((96, size), F32)], axis=0)
            xb[0, c, sub, 1024:] = jnp.transpose(full).astype(BF)
            go(FAR, *at)
            go(NEAR, *at)

    def hand_on(c):
        for at in pieces(PASS, c):
            arrive(FAR, *at)
            go(PASS, *at)

    def ready(c):
        for at in pieces(NEAR, c):
            arrive(NEAR, *at)
            arrive(PASS, *at)

    def give_back(c):
        for at in pieces(BACK3, c):
            go(BACK3, *at)
        for at in pieces(BACK1, c):
            go(BACK1, *at)

    def far_sum(c):
        for at in pieces(BACKX, c):
            arrive(BACK3, *at)
            sub, _ = rows_of(*at)
            fb[c, sub, :] = (ob[2, c, sub, :].astype(F32) + rb[1, c, sub, :].astype(F32)).astype(BF)
            go(BACKX, *at)

    def all_sum(c):
        for at in pieces(BACKY, c):
            arrive(BACK1, *at)
            arrive(BACKX, *at)
            sub, _ = rows_of(*at)
            tb[c, sub, :] = (ob[0, c, sub, :].astype(F32) + rb[0, c, sub, :].astype(F32) + rf[c, sub, :].astype(F32)).astype(BF)
            go(BACKY, *at)

    def last_sum(c):
        for at in pieces(BACKY, c):
            arrive(BACKY, *at)
            sub, span = rows_of(*at)
            moe = tb[c, sub, :].astype(F32) + ry[c, sub, :].astype(F32)
            out_ref[span, :] = (x1[span, :].astype(F32) + moe).astype(BF)

    for c in range(n_c):
        for at in pieces(PART, c):
            go(PART, *at)
    mid(0)
    mid(1)
    hand_on(0)
    for one in loads:
        one.wait()
    table = {
        0: [(ready, 0)], 1: [(mid, 2)], 3: [(hand_on, 1)],
        4: [(give_back, 0), (ready, 1)], 5: [(mid, 3)], 6: [(far_sum, 0)], 7: [(hand_on, 2)],
        8: [(give_back, 1), (ready, 2)], 10: [(far_sum, 1)], 11: [(hand_on, 3)],
        12: [(give_back, 2), (ready, 3)], 13: [(all_sum, 0)], 14: [(far_sum, 2)],
    }
    parts = 4
    lane = lax.broadcasted_iota(jnp.int32, (4 * rows, 128), 1)

    def step(s, carry):
        for k, acts in table.items():
            @pl.when(s == k)
            def _():
                for act, c in acts:
                    act(c)
        c, q = s // parts, lax.rem(s, parts)

        @pl.when(q == 0)
        def _():
            acc[...] = jnp.zeros_like(acc)

        x = jnp.concatenate([xb[n, c, :, :1024] for n in range(4)], axis=0)
        gates = jnp.concatenate([xb[n, c, :, 1024:] for n in range(4)], axis=0).astype(F32)
        total = None
        for m in range(n_e // parts):
            e = q * (n_e // parts) + m
            gate = jnp.dot(x, wg[e], preferred_element_type=F32)
            up = jnp.dot(x, wu[e], preferred_element_type=F32)
            act = (gate * jax.nn.sigmoid(gate) * up).astype(BF)
            y = jnp.dot(act, wd[e], preferred_element_type=F32)
            g_one = jnp.sum(jnp.where(lane == me_ep * n_e + e, gates, 0.0), axis=-1, keepdims=True)
            acc[...] += g_one * y

        @pl.when(q == parts - 1)
        def _():
            for n in range(4):
                ob[n, c] = acc[n * rows:(n + 1) * rows, :].astype(BF)
        return carry

    lax.fori_loop(0, n_c * parts, step, 0)
    give_back(3)
    all_sum(1)
    far_sum(3)
    all_sum(2)
    last_sum(0)
    last_sum(1)
    all_sum(3)
    last_sum(2)
    last_sum(3)
    for kind in range(8):
        for c in range(n_c):
            for at in pieces(kind, c):
                move(kind, *at).wait_send()


def moe_layer(hidden, part, b_out, s2, b2, wr_t, ids, wg, wu, wd):
    n_batch = hidden.shape[0]
    rows = n_batch // CHUNKS
    vmem = pl.BlockSpec(memory_space=pltpu.VMEM)
    hbm = pl.BlockSpec(memory_space=pl.ANY)
    blocks = lambda *lead: pltpu.VMEM(lead + (CHUNKS, rows, 1024), BF)
    return pl.pallas_call(
        moe_kernel,
        in_specs=[vmem] * 7 + [hbm] * 3, out_specs=vmem,
        out_shape=jax.ShapeDtypeStruct((n_batch, 1024), BF),
        scratch_shapes=[
            pltpu.VMEM((n_batch, 1024), BF), pltpu.VMEM((n_batch, 1024), BF), pltpu.VMEM((4, CHUNKS, rows, WIDE), BF),
            pltpu.VMEM(wg.shape, BF), pltpu.VMEM(wu.shape, BF), pltpu.VMEM(wd.shape, BF),
            pltpu.VMEM((4 * rows, 1024), F32), blocks(4), blocks(2), blocks(), blocks(), blocks(), blocks(),
            pltpu.SemaphoreType.DMA((3,)), pltpu.SemaphoreType.DMA((8, 4 * CHUNKS)), pltpu.SemaphoreType.DMA((8, 4 * CHUNKS))],
        compiler_params=pltpu.CompilerParams(collective_id=0, has_side_effects=True, vmem_limit_bytes=VMEM_LIMIT),
        cost_estimate=pl.CostEstimate(flops=26_000_000_000, bytes_accessed=14_000_000, transcendentals=0),
        name="moe",
    )(part, hidden, b_out, s2, b2, wr_t, ids, wg, wu, wd)


def solution(mesh):
    token_rows = P(('dp', 'ep'), None)
    token_vec = P(('dp', 'ep'))
    cache_spec = P(('dp', 'ep'), None, 'tp', None)
    expert_in = P('ep', None, 'tp')
    expert_down = P('ep', 'tp', None)

    def device_step(hidden, seq_lens, rope_cos, rope_sin, ln1_scale, ln1_bias, w_qkv, b_qkv, w_out, b_out, k_cache, v_cache, ln2_scale, ln2_bias, w_router, expert_ids, w_gate, w_up, w_down):
        n_batch = hidden.shape[0]
        kt, vt = (jnp.transpose(c, (0, 2, 3, 1)) for c in (k_cache, v_cache))
        part, *caches = attention(0, n_batch, seq_lens, hidden, rope_cos.T, rope_sin.T, ln1_scale, ln1_bias, w_qkv, b_qkv, w_out, kt, vt, None)
        out = moe_layer(hidden, part, b_out, ln2_scale, ln2_bias, w_router.T, expert_ids.T, w_gate, w_up, w_down)
        return out, *(jnp.transpose(c, (0, 3, 1, 2)) for c in caches)

    in_specs = (token_rows, token_vec, token_rows, token_rows, P(), P(), P(None, 'tp'), P('tp'), P('tp', None), P(), cache_spec, cache_spec, P(), P(), P(), token_rows, expert_in, expert_in, expert_down)
    step = jax.shard_map(device_step, mesh=mesh, in_specs=in_specs, out_specs=(token_rows, cache_spec, cache_spec), check_vma=False)
    return step
```

```python
import functools

import jax
import jax.numpy as jnp
from jax import lax
from jax.experimental import pallas as pl
from jax.experimental.pallas import tpu as pltpu
from jax.sharding import PartitionSpec as P

EPS = 1e-5
BF = jnp.bfloat16
F32 = jnp.float32
CHUNKS = 4
HEAD = 2
TAIL = 4
SUB = 128
BB = 16
WIDE = 1024 + 128
SLOTS = 8
AHEAD = 5
VMEM_LIMIT = 60 * 1024 * 1024


def norm_rows(x, scale, bias):
    mean = jnp.mean(x, axis=-1, keepdims=True)
    cen = x - mean
    var = jnp.mean(cen * cen, axis=-1, keepdims=True)
    return (cen * lax.rsqrt(var + EPS) * scale + bias).astype(BF)


def wide(ref):
    return ref[...].astype(F32).reshape(1, -1)


def attention_kernel(base_row, has_prev, len_ref, hid_ref, cos_ref, sin_ref, s1_ref, b1_ref, bqkv_ref, wqkv_hbm, wout_hbm, k_hbm, v_hbm, *rest):
    part_ref, ko_hbm, vo_hbm = rest[2 * has_prev:2 * has_prev + 3]
    wqkv_ref, wout_ref, kb_ref, vb_ref, qs_ref, kt_ref, vt_ref, sc_ref, pr_ref, cx_ref, ctx_ref, in_sem, out_sem, w_sem = rest[2 * has_prev + 3:]
    step = pl.program_id(0)
    n_step = pl.num_programs(0)
    per_sub = SUB // BB
    j = lax.rem(step, per_sub)
    lane = lax.broadcasted_iota(jnp.int32, (SUB, 128), 1)
    low = lane < 64

    def moves(s, out):
        slot = lax.rem(s, SLOTS)
        src = pl.ds(base_row + s * BB, BB)
        pairs = ((k_hbm, kb_ref, ko_hbm, 0), (v_hbm, vb_ref, vo_hbm, 1))
        if out:
            return [(pltpu.make_async_copy(buf.at[slot], dst.at[src], out_sem.at[t, slot]), t) for _, buf, dst, t in pairs]
        return [(pltpu.make_async_copy(hbm.at[src], buf.at[slot], in_sem.at[t, slot]), t) for hbm, buf, _, t in pairs]

    def begin(s, out):
        for copy, t in moves(s, out):
            copy.start(priority=t)

    def finish(s, out):
        for copy, _ in moves(s, out):
            copy.wait()

    load_qkv = pltpu.make_async_copy(wqkv_hbm, wqkv_ref, w_sem.at[0])
    load_out = pltpu.make_async_copy(wout_hbm, wout_ref, w_sem.at[1])

    @pl.when(step == 0)
    def _():
        load_qkv.start()
        for s in range(AHEAD):
            begin(s, False)
        load_out.start()
        load_qkv.wait()

    @pl.when(j == 0)
    def _():
        normed = norm_rows(hid_ref[...].astype(F32), wide(s1_ref), wide(b1_ref))
        qkv = jnp.dot(normed, wqkv_ref[...], preferred_element_type=F32) + wide(bqkv_ref)
        qkv = qkv.astype(BF).astype(F32)
        col = [qkv[:, m * 128:(m + 1) * 128] for m in range(8)]
        rol = [pltpu.roll(c, 64, 1) for c in col]

        def first(a, b):
            return jnp.where(low, col[a], rol[b])

        def second(a, b):
            return jnp.where(low, rol[a], col[b])

        cos_t, sin_t = cos_ref[...], sin_ref[...]
        cos = jnp.transpose(jnp.concatenate([cos_t] * 4, axis=0))
        sin = jnp.transpose(jnp.concatenate([-sin_t, sin_t] * 2, axis=0))

        def rope(x):
            other = jnp.where(lane % 64 < 32, pltpu.roll(x, 96, 1), pltpu.roll(x, 32, 1))
            return (x * cos + other * sin).astype(BF).astype(F32)

        for h in range(2):
            q0 = rope(first(4 * h, 4 * h + 2))
            q1 = rope(second(4 * h, 4 * h + 2))
            kk = rope(first(4 * h + 1, 4 * h + 3))
            vv = second(4 * h + 1, 4 * h + 3)
            kt_ref[h * 128:(h + 1) * 128, :] = jnp.transpose(kk)
            vt_ref[h * 128:(h + 1) * 128, :] = jnp.transpose(vv)
            for r in range(8):
                src = q0 if r % 2 == 0 else q1
                if r // 4 == h:
                    src = jnp.where(low if (r // 2) % 2 == 0 else ~low, src, 0.0)
                else:
                    src = jnp.zeros_like(src)
                qs_ref[pl.ds(h * SUB * 8 + r, SUB, stride=8), :] = src

    slot = lax.rem(step, SLOTS)
    finish(step, False)
    shift = lax.rem(SUB - j * BB, SUB)
    kt = pltpu.roll(kt_ref[...], shift, 1)
    vt = pltpu.roll(vt_ref[...], shift, 1)[:, :BB].astype(BF)
    unit_row = lax.broadcasted_iota(jnp.int32, (BB, 256), 0)
    unit_col = lax.broadcasted_iota(jnp.int32, (BB, 256), 1) // 128
    lane8 = lax.broadcasted_iota(jnp.int32, (8, 128), 1)
    lane256 = lax.broadcasted_iota(jnp.int32, (256, 128), 1)
    row0 = pl.multiple_of(j * BB * 8, BB * 8)
    base = base_row + step * BB

    def placed(buf, cols, b):
        pos = len_ref[base + b]
        old = buf[slot, b].reshape(256, 128).astype(F32)
        new = jnp.where(lane256 == pos, cols, old).astype(BF)
        buf[slot, b] = new.reshape(4, 64, 128)
        return pos, new

    for b in range(BB):
        pos, k_new = placed(kb_ref, kt[:, b:b + 1], b)
        q_one = jnp.concatenate([qs_ref[pl.ds(row0 + h * SUB * 8 + b * 8, 8), :] for h in range(2)], axis=1).astype(BF)
        s_one = jnp.dot(q_one, k_new, preferred_element_type=F32) * 0.125
        sc_ref[b * 8:(b + 1) * 8, :] = jnp.where(lane8 <= pos, s_one, -jnp.inf)
    s_all = sc_ref[...]
    e_all = jnp.exp(s_all - jnp.max(s_all, axis=-1, keepdims=True))
    pr_ref[...] = e_all / jnp.sum(e_all, axis=-1, keepdims=True)
    for b in range(BB):
        if b % 2 == 0:
            unit = (unit_row == unit_col + b).astype(F32).astype(BF)
            two = jnp.dot(vt, unit, preferred_element_type=F32)
        _, v_new = placed(vb_ref, two[:, (b % 2) * 128:(b % 2 + 1) * 128], b)
        p_one = pr_ref[b * 8:(b + 1) * 8, :].astype(BF)
        c_one = lax.dot_general(p_one, v_new, (((1,), (1,)), ((), ())), preferred_element_type=F32)
        cx_ref[b * 8:(b + 1) * 8, :] = c_one[:, :128]
        cx_ref[BB * 8 + b * 8:BB * 8 + (b + 1) * 8, :] = c_one[:, 128:]
    low_b = lax.broadcasted_iota(jnp.int32, (BB, 128), 1) < 64
    for h in range(2):
        for g in range(2):
            r = 4 * h + 2 * g
            one = cx_ref[pl.ds(h * BB * 8 + r, BB, stride=8), :]
            two = cx_ref[pl.ds(h * BB * 8 + r + 1, BB, stride=8), :]
            if g == 0:
                both = jnp.where(low_b, one, pltpu.roll(two, 64, 1))
            else:
                both = jnp.where(low_b, pltpu.roll(one, 64, 1), two)
            ctx_ref[pl.ds(pl.multiple_of(j * BB, BB), BB), (2 * h + g) * 128:(2 * h + g + 1) * 128] = both.astype(BF)

    begin(step, True)

    @pl.when(step + AHEAD < n_step)
    def _():
        @pl.when(step + AHEAD >= SLOTS)
        def _():
            finish(step + AHEAD - SLOTS, True)
        begin(step + AHEAD, False)

    @pl.when(step == per_sub - 1)
    def _():
        load_out.wait()

    @pl.when(j == per_sub - 1)
    def _():
        part_ref[...] = jnp.dot(ctx_ref[...], wout_ref[...], preferred_element_type=F32).astype(BF)

    @pl.when(step == n_step - 1)
    def _():
        for back in range(SLOTS - 1, -1, -1):
            @pl.when(step >= back)
            def _():
                finish(step - back, True)


def attention(chunk, rows, lens, hidden, cos_t, sin_t, s1, b1, wqkv, bqkv, wout, kt, vt, prev):
    per_sub = SUB // BB
    n_step = rows // BB
    first = chunk * rows // SUB
    vec = pl.BlockSpec((1024,), lambda i, s: (0,))
    hbm = pl.BlockSpec(memory_space=pl.ANY)
    in_specs = [
        pl.BlockSpec((SUB, 1024), lambda i, s: (first + i // per_sub, 0)),
        pl.BlockSpec((32, SUB), lambda i, s: (0, first + i // per_sub)),
        pl.BlockSpec((32, SUB), lambda i, s: (0, first + i // per_sub)),
        vec, vec, vec, hbm, hbm, hbm, hbm,
    ]
    args = [lens, hidden, cos_t, sin_t, s1, b1, bqkv, wqkv, wout, kt, vt]
    aliases = {}
    if prev is not None:
        in_specs += [hbm, hbm]
        aliases = {len(args): 1, len(args) + 1: 2}
        args += list(prev)
    return pl.pallas_call(
        functools.partial(attention_kernel, chunk * rows, int(prev is not None)),
        grid_spec=pltpu.PrefetchScalarGridSpec(
            num_scalar_prefetch=1, grid=(n_step,), in_specs=in_specs,
            out_specs=[pl.BlockSpec((SUB, 1024), lambda i, s: (i // per_sub, 0)), hbm, hbm],
            scratch_shapes=[
                pltpu.VMEM(wqkv.shape, BF), pltpu.VMEM(wout.shape, BF),
                pltpu.VMEM((SLOTS, BB, 4, 64, 128), BF), pltpu.VMEM((SLOTS, BB, 4, 64, 128), BF),
                pltpu.VMEM((2 * SUB * 8, 128), F32), pltpu.VMEM((256, SUB), F32), pltpu.VMEM((256, SUB), F32),
                pltpu.VMEM((BB * 8, 128), F32), pltpu.VMEM((BB * 8, 128), F32),
                pltpu.VMEM((2 * BB * 8, 128), F32), pltpu.VMEM((SUB, 512), BF),
                pltpu.SemaphoreType.DMA((2, SLOTS)), pltpu.SemaphoreType.DMA((2, SLOTS)), pltpu.SemaphoreType.DMA((2,))]),
        out_shape=[jax.ShapeDtypeStruct((rows, 1024), BF), jax.ShapeDtypeStruct(kt.shape, BF), jax.ShapeDtypeStruct(vt.shape, BF)],
        input_output_aliases=aliases,
        compiler_params=pltpu.CompilerParams(dimension_semantics=("arbitrary",), vmem_limit_bytes=VMEM_LIMIT),
        cost_estimate=pl.CostEstimate(flops=rows * 20_000_000, bytes_accessed=rows * 262144, transcendentals=0),
        name="attention",
    )(*args)


PART, NEAR, FAR, PASS, BACK1, BACK3, BACKX, BACKY = range(8)


def moe_kernel(part_ref, hid_ref, bo_ref, s2_ref, b2_ref, wr_ref, ids_ref, wg_hbm, wu_hbm, wd_hbm, out_ref,
               other, x1, xb, wg, wu, wd, acc, ob, rb, fb, rf, tb, ry, w_sem, send, recv):
    me_ep, me_tp = lax.axis_index("ep"), lax.axis_index("tp")
    near = me_ep + 1 - 2 * lax.rem(me_ep, 2)
    far = lax.rem(me_ep + 2, 4)
    peer = 1 - me_tp
    barrier = pltpu.get_barrier_semaphore()
    for dev in ({"ep": near}, {"ep": far}, {"tp": peer}):
        pl.semaphore_signal(barrier, inc=1, device_id=dev, device_id_type=pl.DeviceIdType.MESH)
    loads = [pltpu.make_async_copy(h, v, w_sem.at[m]) for m, (h, v) in enumerate(((wg_hbm, wg), (wu_hbm, wu), (wd_hbm, wd)))]
    for one in loads:
        one.start()
    pl.semaphore_wait(barrier, 3)
    n_c = xb.shape[1]
    rows = xb.shape[2]
    n_e = wg.shape[0]

    split = {0: HEAD, n_c - 1: TAIL}

    def pieces(kind, c):
        early = kind in (PART, NEAR, FAR, PASS)
        count = split.get(c, 1) if (c == 0) == early else 1
        return [(c, p, count) for p in range(count)]

    def move(kind, c, p, count):
        size = rows // count
        sub = pl.ds(p * size, size)
        span = pl.ds(c * rows + p * size, size)
        src, dst, dev = {
            PART: (part_ref.at[span], other.at[span], {"tp": peer}),
            NEAR: (xb.at[0, c, sub], xb.at[1, c, sub], {"ep": near}),
            FAR: (xb.at[0, c, sub], xb.at[2, c, sub], {"ep": far}),
            PASS: (xb.at[2, c, sub], xb.at[3, c, sub], {"ep": near}),
            BACK1: (ob.at[1, c, sub], rb.at[0, c, sub], {"ep": near}),
            BACK3: (ob.at[3, c, sub], rb.at[1, c, sub], {"ep": near}),
            BACKX: (fb.at[c, sub], rf.at[c, sub], {"ep": far}),
            BACKY: (tb.at[c, sub], ry.at[c, sub], {"tp": peer}),
        }[kind]
        lane = p * n_c + c
        return pltpu.make_async_remote_copy(src_ref=src, dst_ref=dst, send_sem=send.at[kind, lane], recv_sem=recv.at[kind, lane], device_id=dev, device_id_type=pl.DeviceIdType.MESH)

    def go(kind, *at):
        move(kind, *at).start()

    def arrive(kind, *at):
        move(kind, *at).wait_recv()

    def rows_of(c, p, count):
        size = rows // count
        return slice(p * size, (p + 1) * size), slice(c * rows + p * size, c * rows + (p + 1) * size)

    def mid(c):
        for at in pieces(FAR, c):
            arrive(PART, *at)
            sub, span = rows_of(*at)
            attn = part_ref[span, :].astype(F32) + other[span, :].astype(F32)
            row = (hid_ref[span, :].astype(F32) + attn + wide(bo_ref)).astype(BF)
            x1[span, :] = row
            h2 = norm_rows(row.astype(F32), wide(s2_ref), wide(b2_ref))
            xb[0, c, sub, :1024] = h2
            size = h2.shape[0]
            logit = lax.dot_general(wr_ref[...], h2, (((1,), (1,)), ((), ())), preferred_element_type=F32)
            eid = lax.broadcasted_iota(jnp.int32, (32, size), 0)
            picked = eid == ids_ref[0:1, span]
            for m in range(1, 8):
                picked = picked | (eid == ids_ref[m:m + 1, span])
            logit = jnp.where(picked, logit, -jnp.inf)
            ex = jnp.exp(logit - jnp.max(logit, axis=0, keepdims=True))
            prob = ex / jnp.sum(ex, axis=0, keepdims=True)
            full = jnp.concatenate([prob, jnp.zeros((96, size), F32)], axis=0)
            xb[0, c, sub, 1024:] = jnp.transpose(full).astype(BF)
            go(FAR, *at)
            go(NEAR, *at)

    def hand_on(c):
        for at in pieces(PASS, c):
            arrive(FAR, *at)
            go(PASS, *at)

    def ready(c):
        for at in pieces(NEAR, c):
            arrive(NEAR, *at)
            arrive(PASS, *at)

    def give_back(c):
        for at in pieces(BACK3, c):
            go(BACK3, *at)
        for at in pieces(BACK1, c):
            go(BACK1, *at)

    def far_sum(c):
        for at in pieces(BACKX, c):
            arrive(BACK3, *at)
            sub, _ = rows_of(*at)
            fb[c, sub, :] = (ob[2, c, sub, :].astype(F32) + rb[1, c, sub, :].astype(F32)).astype(BF)
            go(BACKX, *at)

    def all_sum(c):
        for at in pieces(BACKY, c):
            arrive(BACK1, *at)
            arrive(BACKX, *at)
            sub, _ = rows_of(*at)
            tb[c, sub, :] = (ob[0, c, sub, :].astype(F32) + rb[0, c, sub, :].astype(F32) + rf[c, sub, :].astype(F32)).astype(BF)
            go(BACKY, *at)

    def last_sum(c):
        for at in pieces(BACKY, c):
            arrive(BACKY, *at)
            sub, span = rows_of(*at)
            moe = tb[c, sub, :].astype(F32) + ry[c, sub, :].astype(F32)
            out_ref[span, :] = (x1[span, :].astype(F32) + moe).astype(BF)

    for c in range(n_c):
        for at in pieces(PART, c):
            go(PART, *at)
    mid(0)
    mid(1)
    hand_on(0)
    for one in loads:
        one.wait()
    table = {
        0: [(ready, 0)], 1: [(mid, 2)], 3: [(hand_on, 1)],
        4: [(give_back, 0), (ready, 1)], 5: [(mid, 3)], 6: [(far_sum, 0)], 7: [(hand_on, 2)],
        8: [(give_back, 1), (ready, 2)], 10: [(far_sum, 1)], 11: [(hand_on, 3)],
        12: [(give_back, 2), (ready, 3)], 13: [(all_sum, 0)], 14: [(far_sum, 2)],
    }
    parts = 4
    unit_row = lax.broadcasted_iota(jnp.int32, (128, 128 * n_e // parts), 0)
    unit_col = lax.broadcasted_iota(jnp.int32, (128, 128 * n_e // parts), 1) // 128

    def step(s, carry):
        for k, acts in table.items():
            @pl.when(s == k)
            def _():
                for act, c in acts:
                    act(c)
        c, q = s // parts, lax.rem(s, parts)

        @pl.when(q == 0)
        def _():
            acc[...] = jnp.zeros_like(acc)

        x = jnp.concatenate([xb[n, c, :, :1024] for n in range(4)], axis=0)
        gates = jnp.concatenate([xb[n, c, :, 1024:] for n in range(4)], axis=0)
        unit = (unit_row == me_ep * n_e + q * (n_e // parts) + unit_col).astype(F32).astype(BF)
        wide_gates = jnp.dot(gates, unit, preferred_element_type=F32)
        for m in range(n_e // parts):
            e = q * (n_e // parts) + m
            gate = jnp.dot(x, wg[e], preferred_element_type=F32)
            up = jnp.dot(x, wu[e], preferred_element_type=F32)
            act = (gate * jax.nn.sigmoid(gate) * up).astype(BF)
            y = jnp.dot(act, wd[e], preferred_element_type=F32)
            acc[...] += jnp.concatenate([wide_gates[:, m * 128:(m + 1) * 128]] * 8, axis=1) * y

        @pl.when(q == parts - 1)
        def _():
            for n in range(4):
                ob[n, c] = acc[n * rows:(n + 1) * rows, :].astype(BF)
        return carry

    lax.fori_loop(0, n_c * parts, step, 0)
    give_back(3)
    all_sum(1)
    far_sum(3)
    all_sum(2)
    last_sum(0)
    last_sum(1)
    all_sum(3)
    last_sum(2)
    last_sum(3)
    for kind in range(8):
        for c in range(n_c):
            for at in pieces(kind, c):
                move(kind, *at).wait_send()


def moe_layer(hidden, part, b_out, s2, b2, wr_t, ids, wg, wu, wd):
    n_batch = hidden.shape[0]
    rows = n_batch // CHUNKS
    vmem = pl.BlockSpec(memory_space=pltpu.VMEM)
    hbm = pl.BlockSpec(memory_space=pl.ANY)
    blocks = lambda *lead: pltpu.VMEM(lead + (CHUNKS, rows, 1024), BF)
    return pl.pallas_call(
        moe_kernel,
        in_specs=[vmem] * 7 + [hbm] * 3, out_specs=vmem,
        out_shape=jax.ShapeDtypeStruct((n_batch, 1024), BF),
        scratch_shapes=[
            pltpu.VMEM((n_batch, 1024), BF), pltpu.VMEM((n_batch, 1024), BF), pltpu.VMEM((4, CHUNKS, rows, WIDE), BF),
            pltpu.VMEM(wg.shape, BF), pltpu.VMEM(wu.shape, BF), pltpu.VMEM(wd.shape, BF),
            pltpu.VMEM((4 * rows, 1024), F32), blocks(4), blocks(2), blocks(), blocks(), blocks(), blocks(),
            pltpu.SemaphoreType.DMA((3,)), pltpu.SemaphoreType.DMA((8, 4 * CHUNKS)), pltpu.SemaphoreType.DMA((8, 4 * CHUNKS))],
        compiler_params=pltpu.CompilerParams(collective_id=0, has_side_effects=True, vmem_limit_bytes=VMEM_LIMIT),
        cost_estimate=pl.CostEstimate(flops=26_000_000_000, bytes_accessed=14_000_000, transcendentals=0),
        name="moe",
    )(part, hidden, b_out, s2, b2, wr_t, ids, wg, wu, wd)


def solution(mesh):
    token_rows = P(('dp', 'ep'), None)
    token_vec = P(('dp', 'ep'))
    cache_spec = P(('dp', 'ep'), None, 'tp', None)
    expert_in = P('ep', None, 'tp')
    expert_down = P('ep', 'tp', None)

    def device_step(hidden, seq_lens, rope_cos, rope_sin, ln1_scale, ln1_bias, w_qkv, b_qkv, w_out, b_out, k_cache, v_cache, ln2_scale, ln2_bias, w_router, expert_ids, w_gate, w_up, w_down):
        n_batch = hidden.shape[0]
        kt, vt = (jnp.transpose(c, (0, 2, 3, 1)) for c in (k_cache, v_cache))
        part, *caches = attention(0, n_batch, seq_lens, hidden, rope_cos.T, rope_sin.T, ln1_scale, ln1_bias, w_qkv, b_qkv, w_out, kt, vt, None)
        out = moe_layer(hidden, part, b_out, ln2_scale, ln2_bias, w_router.T, expert_ids.T, w_gate, w_up, w_down)
        return out, *(jnp.transpose(c, (0, 3, 1, 2)) for c in caches)

    in_specs = (token_rows, token_vec, token_rows, token_rows, P(), P(), P(None, 'tp'), P('tp'), P('tp', None), P(), cache_spec, cache_spec, P(), P(), P(), token_rows, expert_in, expert_in, expert_down)
    step = jax.shard_map(device_step, mesh=mesh, in_specs=in_specs, out_specs=(token_rows, cache_spec, cache_spec), check_vma=False)
    return step
```

```python
import functools

import jax
import jax.numpy as jnp
from jax import lax
from jax.experimental import pallas as pl
from jax.experimental.pallas import tpu as pltpu
from jax.sharding import PartitionSpec as P

EPS = 1e-5
BF = jnp.bfloat16
F32 = jnp.float32
CHUNKS = 4
HEAD = 2
TAIL = 4
SUB = 128
BB = 16
WIDE = 1024 + 128
SLOTS = 8
AHEAD = 5
VMEM_LIMIT = 60 * 1024 * 1024


def norm_rows(x, scale, bias):
    mean = jnp.mean(x, axis=-1, keepdims=True)
    cen = x - mean
    var = jnp.mean(cen * cen, axis=-1, keepdims=True)
    return (cen * lax.rsqrt(var + EPS) * scale + bias).astype(BF)


def wide(ref):
    return ref[...].astype(F32).reshape(1, -1)


def attention_kernel(base_row, has_prev, len_ref, hid_ref, cos_ref, sin_ref, s1_ref, b1_ref, bqkv_ref, wqkv_hbm, wout_hbm, k_hbm, v_hbm, *rest):
    part_ref, ko_hbm, vo_hbm = rest[2 * has_prev:2 * has_prev + 3]
    wqkv_ref, wout_ref, kb_ref, vb_ref, qs_ref, kt_ref, vt_ref, sc_ref, pr_ref, cx_ref, ctx_ref, in_sem, out_sem, w_sem = rest[2 * has_prev + 3:]
    step = pl.program_id(0)
    n_step = pl.num_programs(0)
    per_sub = SUB // BB
    j = lax.rem(step, per_sub)
    lane = lax.broadcasted_iota(jnp.int32, (SUB, 128), 1)
    low = lane < 64

    def moves(s, out):
        slot = lax.rem(s, SLOTS)
        src = pl.ds(base_row + s * BB, BB)
        pairs = ((k_hbm, kb_ref, ko_hbm, 0), (v_hbm, vb_ref, vo_hbm, 1))
        if out:
            return [(pltpu.make_async_copy(buf.at[slot], dst.at[src], out_sem.at[t, slot]), t) for _, buf, dst, t in pairs]
        return [(pltpu.make_async_copy(hbm.at[src], buf.at[slot], in_sem.at[t, slot]), t) for hbm, buf, _, t in pairs]

    def begin(s, out):
        for copy, t in moves(s, out):
            copy.start(priority=t)

    def finish(s, out):
        for copy, _ in moves(s, out):
            copy.wait()

    load_qkv = pltpu.make_async_copy(wqkv_hbm, wqkv_ref, w_sem.at[0])
    load_out = pltpu.make_async_copy(wout_hbm, wout_ref, w_sem.at[1])

    @pl.when(step == 0)
    def _():
        load_qkv.start()
        for s in range(AHEAD):
            begin(s, False)
        load_out.start()
        load_qkv.wait()

    @pl.when(j == 0)
    def _():
        normed = norm_rows(hid_ref[...].astype(F32), wide(s1_ref), wide(b1_ref))
        qkv = jnp.dot(normed, wqkv_ref[...], preferred_element_type=F32) + wide(bqkv_ref)
        qkv = qkv.astype(BF).astype(F32)
        col = [qkv[:, m * 128:(m + 1) * 128] for m in range(8)]
        rol = [pltpu.roll(c, 64, 1) for c in col]

        def first(a, b):
            return jnp.where(low, col[a], rol[b])

        def second(a, b):
            return jnp.where(low, rol[a], col[b])

        cos_t, sin_t = cos_ref[...], sin_ref[...]
        cos = jnp.transpose(jnp.concatenate([cos_t] * 4, axis=0))
        sin = jnp.transpose(jnp.concatenate([-sin_t, sin_t] * 2, axis=0))

        def rope(x):
            other = jnp.where(lane % 64 < 32, pltpu.roll(x, 96, 1), pltpu.roll(x, 32, 1))
            return (x * cos + other * sin).astype(BF).astype(F32)

        for h in range(2):
            q0 = rope(first(4 * h, 4 * h + 2))
            q1 = rope(second(4 * h, 4 * h + 2))
            kk = rope(first(4 * h + 1, 4 * h + 3))
            vv = second(4 * h + 1, 4 * h + 3)
            kt_ref[h * 128:(h + 1) * 128, :] = jnp.transpose(kk)
            vt_ref[h * 128:(h + 1) * 128, :] = jnp.transpose(vv)
            for r in range(8):
                src = q0 if r % 2 == 0 else q1
                if r // 4 == h:
                    src = jnp.where(low if (r // 2) % 2 == 0 else ~low, src, 0.0)
                else:
                    src = jnp.zeros_like(src)
                qs_ref[pl.ds(h * SUB * 8 + r, SUB, stride=8), :] = src

    slot = lax.rem(step, SLOTS)
    finish(step, False)
    shift = lax.rem(SUB - j * BB, SUB)
    kt = pltpu.roll(kt_ref[...], shift, 1)
    vt = pltpu.roll(vt_ref[...], shift, 1)[:, :BB].astype(BF)
    unit_row = lax.broadcasted_iota(jnp.int32, (BB, 256), 0)
    unit_col = lax.broadcasted_iota(jnp.int32, (BB, 256), 1) // 128
    lane8 = lax.broadcasted_iota(jnp.int32, (8, 128), 1)
    lane256 = lax.broadcasted_iota(jnp.int32, (256, 128), 1)
    row0 = pl.multiple_of(j * BB * 8, BB * 8)
    base = base_row + step * BB

    def placed(buf, cols, b):
        pos = len_ref[base + b]
        old = buf[slot, b].reshape(256, 128).astype(F32)
        new = jnp.where(lane256 == pos, cols, old).astype(BF)
        buf[slot, b] = new.reshape(4, 64, 128)
        return pos, new

    for b in range(BB):
        pos, k_new = placed(kb_ref, kt[:, b:b + 1], b)
        q_one = jnp.concatenate([qs_ref[pl.ds(row0 + h * SUB * 8 + b * 8, 8), :] for h in range(2)], axis=1).astype(BF)
        s_one = jnp.dot(q_one, k_new, preferred_element_type=F32) * 0.125
        sc_ref[b * 8:(b + 1) * 8, :] = jnp.where(lane8 <= pos, s_one, -jnp.inf)
    s_all = sc_ref[...]
    e_all = jnp.exp(s_all - jnp.max(s_all, axis=-1, keepdims=True))
    pr_ref[...] = e_all / jnp.sum(e_all, axis=-1, keepdims=True)
    for b in range(BB):
        if b % 2 == 0:
            unit = (unit_row == unit_col + b).astype(F32).astype(BF)
            two = jnp.dot(vt, unit, preferred_element_type=F32)
        _, v_new = placed(vb_ref, two[:, (b % 2) * 128:(b % 2 + 1) * 128], b)
        p_one = pr_ref[b * 8:(b + 1) * 8, :].astype(BF)
        c_one = lax.dot_general(p_one, v_new, (((1,), (1,)), ((), ())), preferred_element_type=F32)
        cx_ref[b * 8:(b + 1) * 8, :] = c_one[:, :128]
        cx_ref[BB * 8 + b * 8:BB * 8 + (b + 1) * 8, :] = c_one[:, 128:]
    low_b = lax.broadcasted_iota(jnp.int32, (BB, 128), 1) < 64
    for h in range(2):
        for g in range(2):
            r = 4 * h + 2 * g
            one = cx_ref[pl.ds(h * BB * 8 + r, BB, stride=8), :]
            two = cx_ref[pl.ds(h * BB * 8 + r + 1, BB, stride=8), :]
            if g == 0:
                both = jnp.where(low_b, one, pltpu.roll(two, 64, 1))
            else:
                both = jnp.where(low_b, pltpu.roll(one, 64, 1), two)
            ctx_ref[pl.ds(pl.multiple_of(j * BB, BB), BB), (2 * h + g) * 128:(2 * h + g + 1) * 128] = both.astype(BF)

    begin(step, True)

    @pl.when(step + AHEAD < n_step)
    def _():
        @pl.when(step + AHEAD >= SLOTS)
        def _():
            finish(step + AHEAD - SLOTS, True)

        begin(step + AHEAD, False)

    @pl.when(step == per_sub - 1)
    def _():
        load_out.wait()

    @pl.when(j == per_sub - 1)
    def _():
        part_ref[...] = jnp.dot(ctx_ref[...], wout_ref[...], preferred_element_type=F32).astype(BF)

    @pl.when(step == n_step - 1)
    def _():
        for back in range(SLOTS - 1, -1, -1):
            @pl.when(step >= back)
            def _():
                finish(step - back, True)


def attention(chunk, rows, lens, hidden, cos_t, sin_t, s1, b1, wqkv, bqkv, wout, kt, vt, prev):
    per_sub = SUB // BB
    n_step = rows // BB
    first = chunk * rows // SUB
    vec = pl.BlockSpec((1024,), lambda i, s: (0,))
    hbm = pl.BlockSpec(memory_space=pl.ANY)
    in_specs = [
        pl.BlockSpec((SUB, 1024), lambda i, s: (first + i // per_sub, 0)),
        pl.BlockSpec((32, SUB), lambda i, s: (0, first + i // per_sub)),
        pl.BlockSpec((32, SUB), lambda i, s: (0, first + i // per_sub)),
        vec, vec, vec, hbm, hbm, hbm, hbm,
    ]
    args = [lens, hidden, cos_t, sin_t, s1, b1, bqkv, wqkv, wout, kt, vt]
    aliases = {}
    if prev is not None:
        in_specs += [hbm, hbm]
        aliases = {len(args): 1, len(args) + 1: 2}
        args += list(prev)
    return pl.pallas_call(
        functools.partial(attention_kernel, chunk * rows, int(prev is not None)),
        grid_spec=pltpu.PrefetchScalarGridSpec(
            num_scalar_prefetch=1, grid=(n_step,), in_specs=in_specs,
            out_specs=[pl.BlockSpec((SUB, 1024), lambda i, s: (i // per_sub, 0)), hbm, hbm],
            scratch_shapes=[
                pltpu.VMEM(wqkv.shape, BF), pltpu.VMEM(wout.shape, BF),
                pltpu.VMEM((SLOTS, BB, 4, 64, 128), BF), pltpu.VMEM((SLOTS, BB, 4, 64, 128), BF),
                pltpu.VMEM((2 * SUB * 8, 128), F32), pltpu.VMEM((256, SUB), F32), pltpu.VMEM((256, SUB), F32),
                pltpu.VMEM((BB * 8, 128), F32), pltpu.VMEM((BB * 8, 128), F32),
                pltpu.VMEM((2 * BB * 8, 128), F32), pltpu.VMEM((SUB, 512), BF),
                pltpu.SemaphoreType.DMA((2, SLOTS)), pltpu.SemaphoreType.DMA((2, SLOTS)), pltpu.SemaphoreType.DMA((2,))]),
        out_shape=[jax.ShapeDtypeStruct((rows, 1024), BF), jax.ShapeDtypeStruct(kt.shape, BF), jax.ShapeDtypeStruct(vt.shape, BF)],
        input_output_aliases=aliases,
        compiler_params=pltpu.CompilerParams(dimension_semantics=("arbitrary",), vmem_limit_bytes=VMEM_LIMIT),
        cost_estimate=pl.CostEstimate(flops=rows * 20_000_000, bytes_accessed=rows * 262144, transcendentals=0),
        name="attention",
    )(*args)


PART, NEAR, FAR, PASS, BACK1, BACK3, BACKX, BACKY = range(8)


def moe_kernel(early_ref, early_other, part_ref, hid_ref, bo_ref, s2_ref, b2_ref, wr_ref, ids_ref, wg_hbm, wu_hbm, wd_hbm, out_ref,
               other, x1, xb, wg, wu, wd, acc, ob, rb, fb, rf, tb, ry, w_sem, send, recv):
    me_ep, me_tp = lax.axis_index("ep"), lax.axis_index("tp")
    near = me_ep + 1 - 2 * lax.rem(me_ep, 2)
    far = lax.rem(me_ep + 2, 4)
    peer = 1 - me_tp
    barrier = pltpu.get_barrier_semaphore()
    for dev in ({"ep": near}, {"ep": far}, {"tp": peer}):
        pl.semaphore_signal(barrier, inc=1, device_id=dev, device_id_type=pl.DeviceIdType.MESH)
    loads = [pltpu.make_async_copy(h, v, w_sem.at[m]) for m, (h, v) in enumerate(((wg_hbm, wg), (wu_hbm, wu), (wd_hbm, wd)))]
    for one in loads:
        one.start()
    pl.semaphore_wait(barrier, 3)
    n_c = xb.shape[1]
    rows = xb.shape[2]
    n_e = wg.shape[0]

    split = {0: HEAD, n_c - 1: TAIL}

    first_late = n_c - part_ref.shape[0] // rows

    def pieces(kind, c):
        if kind == PART and c < first_late:
            return []
        early = kind in (PART, NEAR, FAR, PASS)
        count = split.get(c, 1) if (c == 0) == early else 1
        return [(c, p, count) for p in range(count)]

    def move(kind, c, p, count):
        size = rows // count
        sub = pl.ds(p * size, size)
        late = pl.ds(max(c - first_late, 0) * rows + p * size, size)
        src, dst, dev = {
            PART: (part_ref.at[late], other.at[late], {"tp": peer}),
            NEAR: (xb.at[0, c, sub], xb.at[1, c, sub], {"ep": near}),
            FAR: (xb.at[0, c, sub], xb.at[2, c, sub], {"ep": far}),
            PASS: (xb.at[2, c, sub], xb.at[3, c, sub], {"ep": near}),
            BACK1: (ob.at[1, c, sub], rb.at[0, c, sub], {"ep": near}),
            BACK3: (ob.at[3, c, sub], rb.at[1, c, sub], {"ep": near}),
            BACKX: (fb.at[c, sub], rf.at[c, sub], {"ep": far}),
            BACKY: (tb.at[c, sub], ry.at[c, sub], {"tp": peer}),
        }[kind]
        lane = p * n_c + c
        return pltpu.make_async_remote_copy(src_ref=src, dst_ref=dst, send_sem=send.at[kind, lane], recv_sem=recv.at[kind, lane], device_id=dev, device_id_type=pl.DeviceIdType.MESH)

    def go(kind, *at):
        move(kind, *at).start()

    def arrive(kind, *at):
        move(kind, *at).wait_recv()

    def rows_of(c, p, count):
        size = rows // count
        return slice(p * size, (p + 1) * size), slice(c * rows + p * size, c * rows + (p + 1) * size)

    def mid(c):
        for at in pieces(FAR, c):
            sub, span = rows_of(*at)
            if c < first_late:
                attn = early_ref[span, :].astype(F32) + early_other[span, :].astype(F32)
            else:
                arrive(PART, *at)
                _, late = rows_of(c - first_late, *at[1:])
                attn = part_ref[late, :].astype(F32) + other[late, :].astype(F32)
            row = (hid_ref[span, :].astype(F32) + attn + wide(bo_ref)).astype(BF)
            x1[span, :] = row
            h2 = norm_rows(row.astype(F32), wide(s2_ref), wide(b2_ref))
            xb[0, c, sub, :1024] = h2
            size = h2.shape[0]
            logit = lax.dot_general(wr_ref[...], h2, (((1,), (1,)), ((), ())), preferred_element_type=F32)
            eid = lax.broadcasted_iota(jnp.int32, (32, size), 0)
            picked = eid == ids_ref[0:1, span]
            for m in range(1, 8):
                picked = picked | (eid == ids_ref[m:m + 1, span])
            logit = jnp.where(picked, logit, -jnp.inf)
            ex = jnp.exp(logit - jnp.max(logit, axis=0, keepdims=True))
            prob = ex / jnp.sum(ex, axis=0, keepdims=True)
            full = jnp.concatenate([prob, jnp.zeros((96, size), F32)], axis=0)
            xb[0, c, sub, 1024:] = jnp.transpose(full).astype(BF)
            go(FAR, *at)
            go(NEAR, *at)

    def hand_on(c):
        for at in pieces(PASS, c):
            arrive(FAR, *at)
            go(PASS, *at)

    def ready(c):
        for at in pieces(NEAR, c):
            arrive(NEAR, *at)
            arrive(PASS, *at)

    def give_back(c):
        for at in pieces(BACK3, c):
            go(BACK3, *at)
        for at in pieces(BACK1, c):
            go(BACK1, *at)

    def far_sum(c):
        for at in pieces(BACKX, c):
            arrive(BACK3, *at)
            sub, _ = rows_of(*at)
            fb[c, sub, :] = (ob[2, c, sub, :].astype(F32) + rb[1, c, sub, :].astype(F32)).astype(BF)
            go(BACKX, *at)

    def all_sum(c):
        for at in pieces(BACKY, c):
            arrive(BACK1, *at)
            arrive(BACKX, *at)
            sub, _ = rows_of(*at)
            tb[c, sub, :] = (ob[0, c, sub, :].astype(F32) + rb[0, c, sub, :].astype(F32) + rf[c, sub, :].astype(F32)).astype(BF)
            go(BACKY, *at)

    def last_sum(c):
        for at in pieces(BACKY, c):
            arrive(BACKY, *at)
            sub, span = rows_of(*at)
            moe = tb[c, sub, :].astype(F32) + ry[c, sub, :].astype(F32)
            out_ref[span, :] = (x1[span, :].astype(F32) + moe).astype(BF)

    for c in range(n_c):
        for at in pieces(PART, c):
            go(PART, *at)
    mid(0)
    mid(1)
    mid(2)
    hand_on(0)
    for one in loads:
        one.wait()
    table = {
        0: [(ready, 0)], 2: [(mid, 3)], 3: [(hand_on, 1)],
        4: [(give_back, 0), (ready, 1)], 5: [(far_sum, 0)], 6: [(hand_on, 2)],
        8: [(give_back, 1), (ready, 2)], 9: [(hand_on, 3), (far_sum, 1)], 11: [(all_sum, 0)],
        12: [(give_back, 2), (ready, 3)], 13: [(far_sum, 2)], 15: [(all_sum, 1)],
    }
    parts = 4
    unit_row = lax.broadcasted_iota(jnp.int32, (128, 128 * n_e // parts), 0)
    unit_col = lax.broadcasted_iota(jnp.int32, (128, 128 * n_e // parts), 1) // 128

    def step(s, carry):
        for k, acts in table.items():
            @pl.when(s == k)
            def _():
                for act, c in acts:
                    act(c)
        c, q = s // parts, lax.rem(s, parts)

        @pl.when(q == 0)
        def _():
            acc[...] = jnp.zeros_like(acc)

        x = jnp.concatenate([xb[n, c, :, :1024] for n in range(4)], axis=0)
        gates = jnp.concatenate([xb[n, c, :, 1024:] for n in range(4)], axis=0)
        unit = (unit_row == me_ep * n_e + q * (n_e // parts) + unit_col).astype(F32).astype(BF)
        wide_gates = jnp.dot(gates, unit, preferred_element_type=F32)
        for m in range(n_e // parts):
            e = q * (n_e // parts) + m
            gate = jnp.dot(x, wg[e], preferred_element_type=F32)
            up = jnp.dot(x, wu[e], preferred_element_type=F32)
            act = (gate * jax.nn.sigmoid(gate) * up).astype(BF)
            y = jnp.dot(act, wd[e], preferred_element_type=F32)
            acc[...] += jnp.concatenate([wide_gates[:, m * 128:(m + 1) * 128]] * 8, axis=1) * y

        @pl.when(q == parts - 1)
        def _():
            for n in range(4):
                ob[n, c] = acc[n * rows:(n + 1) * rows, :].astype(BF)

        return carry

    lax.fori_loop(0, n_c * parts, step, 0)
    give_back(3)
    far_sum(3)
    all_sum(2)
    last_sum(0)
    last_sum(1)
    all_sum(3)
    last_sum(2)
    last_sum(3)
    for kind in range(8):
        for c in range(n_c):
            for at in pieces(kind, c):
                move(kind, *at).wait_send()


def moe_layer(hidden, early, early_other, part, b_out, s2, b2, wr_t, ids, wg, wu, wd):
    n_batch = hidden.shape[0]
    rows = n_batch // CHUNKS
    vmem = pl.BlockSpec(memory_space=pltpu.VMEM)
    hbm = pl.BlockSpec(memory_space=pl.ANY)
    blocks = lambda *lead: pltpu.VMEM(lead + (CHUNKS, rows, 1024), BF)
    return pl.pallas_call(
        moe_kernel,
        in_specs=[vmem] * 9 + [hbm] * 3, out_specs=vmem,
        out_shape=jax.ShapeDtypeStruct((n_batch, 1024), BF),
        scratch_shapes=[
            pltpu.VMEM(part.shape, BF), pltpu.VMEM((n_batch, 1024), BF), pltpu.VMEM((4, CHUNKS, rows, WIDE), BF),
            pltpu.VMEM(wg.shape, BF), pltpu.VMEM(wu.shape, BF), pltpu.VMEM(wd.shape, BF),
            pltpu.VMEM((4 * rows, 1024), F32), blocks(4), blocks(2), blocks(), blocks(), blocks(), blocks(),
            pltpu.SemaphoreType.DMA((3,)), pltpu.SemaphoreType.DMA((8, 4 * CHUNKS)), pltpu.SemaphoreType.DMA((8, 4 * CHUNKS))],
        compiler_params=pltpu.CompilerParams(collective_id=0, has_side_effects=True, vmem_limit_bytes=VMEM_LIMIT),
        cost_estimate=pl.CostEstimate(flops=26_000_000_000, bytes_accessed=14_000_000, transcendentals=0),
        name="moe",
    )(early, early_other, part, hidden, b_out, s2, b2, wr_t, ids, wg, wu, wd)


def solution(mesh):
    token_rows = P(('dp', 'ep'), None)
    token_vec = P(('dp', 'ep'))
    cache_spec = P(('dp', 'ep'), None, 'tp', None)
    expert_in = P('ep', None, 'tp')
    expert_down = P('ep', 'tp', None)

    def device_step(hidden, seq_lens, rope_cos, rope_sin, ln1_scale, ln1_bias, w_qkv, b_qkv, w_out, b_out, k_cache, v_cache, ln2_scale, ln2_bias, w_router, expert_ids, w_gate, w_up, w_down):
        n_batch = hidden.shape[0]
        kt, vt = (jnp.transpose(c, (0, 2, 3, 1)) for c in (k_cache, v_cache))
        half = n_batch // 2
        caches, parts = None, []
        for c in range(2):
            part, *caches = attention(c, half, seq_lens, hidden, rope_cos.T, rope_sin.T, ln1_scale, ln1_bias, w_qkv, b_qkv, w_out, kt, vt, caches)
            parts.append(part)
            if c == 0:
                other = lax.ppermute(part, 'tp', [(0, 1), (1, 0)])
        out = moe_layer(hidden, parts[0], other, parts[1], b_out, ln2_scale, ln2_bias, w_router.T, expert_ids.T, w_gate, w_up, w_down)
        return out, *(jnp.transpose(c, (0, 3, 1, 2)) for c in caches)

    in_specs = (token_rows, token_vec, token_rows, token_rows, P(), P(), P(None, 'tp'), P('tp'), P('tp', None), P(), cache_spec, cache_spec, P(), P(), P(), token_rows, expert_in, expert_in, expert_down)
    return jax.shard_map(device_step, mesh=mesh, in_specs=in_specs, out_specs=(token_rows, cache_spec, cache_spec), check_vma=False)
```

```python
import functools

import jax
import jax.numpy as jnp
from jax import lax
from jax.experimental import pallas as pl
from jax.experimental.pallas import tpu as pltpu
from jax.sharding import PartitionSpec as P

EPS = 1e-5
BF = jnp.bfloat16
F32 = jnp.float32
CHUNKS = 4
HEAD = 2
TAIL = 4
SUB = 128
BB = 32
WIDE = 1024 + 128
SLOTS = 5
AHEAD = 3
VMEM_LIMIT = 60 * 1024 * 1024


def norm_rows(x, scale, bias):
    mean = jnp.mean(x, axis=-1, keepdims=True)
    cen = x - mean
    var = jnp.mean(cen * cen, axis=-1, keepdims=True)
    return (cen * lax.rsqrt(var + EPS) * scale + bias).astype(BF)


def wide(ref):
    return ref[...].astype(F32).reshape(1, -1)


def attention_kernel(base_row, has_prev, len_ref, hid_ref, cos_ref, sin_ref, s1_ref, b1_ref, bqkv_ref, wqkv_hbm, wout_hbm, k_hbm, v_hbm, *rest):
    part_ref, ko_hbm, vo_hbm = rest[2 * has_prev:2 * has_prev + 3]
    wqkv_ref, wout_ref, kb_ref, vb_ref, qs_ref, kt_ref, vt_ref, sc_ref, pr_ref, cx_ref, ctx_ref, in_sem, out_sem, w_sem = rest[2 * has_prev + 3:]
    step = pl.program_id(0)
    n_step = pl.num_programs(0)
    per_sub = SUB // BB
    j = lax.rem(step, per_sub)
    lane = lax.broadcasted_iota(jnp.int32, (SUB, 128), 1)
    low = lane < 64

    def moves(s, out):
        slot = lax.rem(s, SLOTS)
        src = pl.ds(base_row + s * BB, BB)
        pairs = ((k_hbm, kb_ref, ko_hbm, 0), (v_hbm, vb_ref, vo_hbm, 1))
        if out:
            return [(pltpu.make_async_copy(buf.at[slot], dst.at[src], out_sem.at[t, slot]), t) for _, buf, dst, t in pairs]
        return [(pltpu.make_async_copy(hbm.at[src], buf.at[slot], in_sem.at[t, slot]), t) for hbm, buf, _, t in pairs]

    def begin(s, out):
        for copy, t in moves(s, out):
            copy.start(priority=t)

    def finish(s, out):
        for copy, _ in moves(s, out):
            copy.wait()

    load_qkv = pltpu.make_async_copy(wqkv_hbm, wqkv_ref, w_sem.at[0])
    load_out = pltpu.make_async_copy(wout_hbm, wout_ref, w_sem.at[1])

    @pl.when(step == 0)
    def _():
        load_qkv.start()
        for s in range(AHEAD):
            begin(s, False)
        load_out.start()
        load_qkv.wait()

    @pl.when(j == 0)
    def _():
        normed = norm_rows(hid_ref[...].astype(F32), wide(s1_ref), wide(b1_ref))
        qkv = jnp.dot(normed, wqkv_ref[...], preferred_element_type=F32) + wide(bqkv_ref)
        qkv = qkv.astype(BF).astype(F32)
        col = [qkv[:, m * 128:(m + 1) * 128] for m in range(8)]
        rol = [pltpu.roll(c, 64, 1) for c in col]

        def first(a, b):
            return jnp.where(low, col[a], rol[b])

        def second(a, b):
            return jnp.where(low, rol[a], col[b])

        cos_t, sin_t = cos_ref[...], sin_ref[...]
        cos = jnp.transpose(jnp.concatenate([cos_t] * 4, axis=0))
        sin = jnp.transpose(jnp.concatenate([-sin_t, sin_t] * 2, axis=0))

        def rope(x):
            other = jnp.where(lane % 64 < 32, pltpu.roll(x, 96, 1), pltpu.roll(x, 32, 1))
            return (x * cos + other * sin).astype(BF).astype(F32)

        for h in range(2):
            q0 = rope(first(4 * h, 4 * h + 2))
            q1 = rope(second(4 * h, 4 * h + 2))
            kk = rope(first(4 * h + 1, 4 * h + 3))
            vv = second(4 * h + 1, 4 * h + 3)
            kt_ref[h * 128:(h + 1) * 128, :] = jnp.transpose(kk)
            vt_ref[h * 128:(h + 1) * 128, :] = jnp.transpose(vv)
            for r in range(8):
                src = q0 if r % 2 == 0 else q1
                if r // 4 == h:
                    src = jnp.where(low if (r // 2) % 2 == 0 else ~low, src, 0.0)
                else:
                    src = jnp.zeros_like(src)
                qs_ref[pl.ds(h * SUB * 8 + r, SUB, stride=8), :] = src

    slot = lax.rem(step, SLOTS)
    finish(step, False)
    shift = lax.rem(SUB - j * BB, SUB)
    kt = pltpu.roll(kt_ref[...], shift, 1)
    vt = pltpu.roll(vt_ref[...], shift, 1)[:, :BB].astype(BF)
    unit_row = lax.broadcasted_iota(jnp.int32, (BB, 256), 0)
    unit_col = lax.broadcasted_iota(jnp.int32, (BB, 256), 1) // 128
    lane8 = lax.broadcasted_iota(jnp.int32, (8, 128), 1)
    lane256 = lax.broadcasted_iota(jnp.int32, (256, 128), 1)
    row0 = pl.multiple_of(j * BB * 8, BB * 8)
    base = base_row + step * BB

    def placed(buf, cols, b):
        pos = len_ref[base + b]
        old = buf[slot, b].reshape(256, 128).astype(F32)
        new = jnp.where(lane256 == pos, cols, old).astype(BF)
        buf[slot, b] = new.reshape(4, 64, 128)
        return pos, new

    for b in range(BB):
        pos, k_new = placed(kb_ref, kt[:, b:b + 1], b)
        q_one = jnp.concatenate([qs_ref[pl.ds(row0 + h * SUB * 8 + b * 8, 8), :] for h in range(2)], axis=1).astype(BF)
        s_one = jnp.dot(q_one, k_new, preferred_element_type=F32) * 0.125
        sc_ref[b * 8:(b + 1) * 8, :] = jnp.where(lane8 <= pos, s_one, -jnp.inf)
    s_all = sc_ref[...]
    e_all = jnp.exp(s_all - jnp.max(s_all, axis=-1, keepdims=True))
    pr_ref[...] = e_all / jnp.sum(e_all, axis=-1, keepdims=True)
    for b in range(BB):
        if b % 2 == 0:
            unit = (unit_row == unit_col + b).astype(F32).astype(BF)
            two = jnp.dot(vt, unit, preferred_element_type=F32)
        _, v_new = placed(vb_ref, two[:, (b % 2) * 128:(b % 2 + 1) * 128], b)
        p_one = pr_ref[b * 8:(b + 1) * 8, :].astype(BF)
        c_one = lax.dot_general(p_one, v_new, (((1,), (1,)), ((), ())), preferred_element_type=F32)
        cx_ref[b * 8:(b + 1) * 8, :] = c_one[:, :128]
        cx_ref[BB * 8 + b * 8:BB * 8 + (b + 1) * 8, :] = c_one[:, 128:]
    low_b = lax.broadcasted_iota(jnp.int32, (BB, 128), 1) < 64
    for h in range(2):
        for g in range(2):
            r = 4 * h + 2 * g
            one = cx_ref[pl.ds(h * BB * 8 + r, BB, stride=8), :]
            two = cx_ref[pl.ds(h * BB * 8 + r + 1, BB, stride=8), :]
            if g == 0:
                both = jnp.where(low_b, one, pltpu.roll(two, 64, 1))
            else:
                both = jnp.where(low_b, pltpu.roll(one, 64, 1), two)
            ctx_ref[pl.ds(pl.multiple_of(j * BB, BB), BB), (2 * h + g) * 128:(2 * h + g + 1) * 128] = both.astype(BF)

    begin(step, True)

    @pl.when(step + AHEAD < n_step)
    def _():
        @pl.when(step + AHEAD >= SLOTS)
        def _():
            finish(step + AHEAD - SLOTS, True)
        begin(step + AHEAD, False)

    @pl.when(step == per_sub - 1)
    def _():
        load_out.wait()

    @pl.when(j == per_sub - 1)
    def _():
        part_ref[...] = jnp.dot(ctx_ref[...], wout_ref[...], preferred_element_type=F32).astype(BF)

    @pl.when(step == n_step - 1)
    def _():
        for back in range(SLOTS - 1, -1, -1):
            @pl.when(step >= back)
            def _():
                finish(step - back, True)


def attention(chunk, rows, lens, hidden, cos_t, sin_t, s1, b1, wqkv, bqkv, wout, kt, vt, prev):
    per_sub = SUB // BB
    n_step = rows // BB
    first = chunk * rows // SUB
    vec = pl.BlockSpec((1024,), lambda i, s: (0,))
    hbm = pl.BlockSpec(memory_space=pl.ANY)
    in_specs = [
        pl.BlockSpec((SUB, 1024), lambda i, s: (first + i // per_sub, 0)),
        pl.BlockSpec((32, SUB), lambda i, s: (0, first + i // per_sub)),
        pl.BlockSpec((32, SUB), lambda i, s: (0, first + i // per_sub)),
        vec, vec, vec, hbm, hbm, hbm, hbm,
    ]
    args = [lens, hidden, cos_t, sin_t, s1, b1, bqkv, wqkv, wout, kt, vt]
    aliases = {}
    if prev is not None:
        in_specs += [hbm, hbm]
        aliases = {len(args): 1, len(args) + 1: 2}
        args += list(prev)
    return pl.pallas_call(
        functools.partial(attention_kernel, chunk * rows, int(prev is not None)),
        grid_spec=pltpu.PrefetchScalarGridSpec(
            num_scalar_prefetch=1, grid=(n_step,), in_specs=in_specs,
            out_specs=[pl.BlockSpec((SUB, 1024), lambda i, s: (i // per_sub, 0)), hbm, hbm],
            scratch_shapes=[
                pltpu.VMEM(wqkv.shape, BF), pltpu.VMEM(wout.shape, BF),
                pltpu.VMEM((SLOTS, BB, 4, 64, 128), BF), pltpu.VMEM((SLOTS, BB, 4, 64, 128), BF),
                pltpu.VMEM((2 * SUB * 8, 128), F32), pltpu.VMEM((256, SUB), F32), pltpu.VMEM((256, SUB), F32),
                pltpu.VMEM((BB * 8, 128), F32), pltpu.VMEM((BB * 8, 128), F32),
                pltpu.VMEM((2 * BB * 8, 128), F32), pltpu.VMEM((SUB, 512), BF),
                pltpu.SemaphoreType.DMA((2, SLOTS)), pltpu.SemaphoreType.DMA((2, SLOTS)), pltpu.SemaphoreType.DMA((2,))]),
        out_shape=[jax.ShapeDtypeStruct((rows, 1024), BF), jax.ShapeDtypeStruct(kt.shape, BF), jax.ShapeDtypeStruct(vt.shape, BF)],
        input_output_aliases=aliases,
        compiler_params=pltpu.CompilerParams(dimension_semantics=("arbitrary",), vmem_limit_bytes=VMEM_LIMIT),
        cost_estimate=pl.CostEstimate(flops=rows * 20_000_000, bytes_accessed=rows * 262144, transcendentals=0),
        name="attention",
    )(*args)


PART, NEAR, FAR, PASS, BACK1, BACK3, BACKX, BACKY = range(8)


def moe_kernel(part_ref, hid_ref, bo_ref, s2_ref, b2_ref, wr_ref, ids_ref, wg_hbm, wu_hbm, wd_hbm, out_ref,
               other, x1, xb, wg, wu, wd, acc, ob, rb, fb, rf, tb, ry, w_sem, send, recv):
    me_ep, me_tp = lax.axis_index("ep"), lax.axis_index("tp")
    near = me_ep + 1 - 2 * lax.rem(me_ep, 2)
    far = lax.rem(me_ep + 2, 4)
    peer = 1 - me_tp
    barrier = pltpu.get_barrier_semaphore()
    for dev in ({"ep": near}, {"ep": far}, {"tp": peer}):
        pl.semaphore_signal(barrier, inc=1, device_id=dev, device_id_type=pl.DeviceIdType.MESH)
    loads = [pltpu.make_async_copy(h, v, w_sem.at[m]) for m, (h, v) in enumerate(((wg_hbm, wg), (wu_hbm, wu), (wd_hbm, wd)))]
    for one in loads:
        one.start()
    pl.semaphore_wait(barrier, 3)
    n_c = xb.shape[1]
    rows = xb.shape[2]
    n_e = wg.shape[0]

    split = {0: HEAD, n_c - 1: TAIL}

    def pieces(kind, c):
        early = kind in (PART, NEAR, FAR, PASS)
        count = split.get(c, 1) if (c == 0) == early else 1
        return [(c, p, count) for p in range(count)]

    def move(kind, c, p, count):
        size = rows // count
        sub = pl.ds(p * size, size)
        span = pl.ds(c * rows + p * size, size)
        src, dst, dev = {
            PART: (part_ref.at[span], other.at[span], {"tp": peer}),
            NEAR: (xb.at[0, c, sub], xb.at[1, c, sub], {"ep": near}),
            FAR: (xb.at[0, c, sub], xb.at[2, c, sub], {"ep": far}),
            PASS: (xb.at[2, c, sub], xb.at[3, c, sub], {"ep": near}),
            BACK1: (ob.at[1, c, sub], rb.at[0, c, sub], {"ep": near}),
            BACK3: (ob.at[3, c, sub], rb.at[1, c, sub], {"ep": near}),
            BACKX: (fb.at[c, sub], rf.at[c, sub], {"ep": far}),
            BACKY: (tb.at[c, sub], ry.at[c, sub], {"tp": peer}),
        }[kind]
        lane = p * n_c + c
        return pltpu.make_async_remote_copy(src_ref=src, dst_ref=dst, send_sem=send.at[kind, lane], recv_sem=recv.at[kind, lane], device_id=dev, device_id_type=pl.DeviceIdType.MESH)

    def go(kind, *at):
        move(kind, *at).start()

    def arrive(kind, *at):
        move(kind, *at).wait_recv()

    def rows_of(c, p, count):
        size = rows // count
        return slice(p * size, (p + 1) * size), slice(c * rows + p * size, c * rows + (p + 1) * size)

    def mid(c):
        for at in pieces(FAR, c):
            arrive(PART, *at)
            sub, span = rows_of(*at)
            attn = part_ref[span, :].astype(F32) + other[span, :].astype(F32)
            row = (hid_ref[span, :].astype(F32) + attn + wide(bo_ref)).astype(BF)
            x1[span, :] = row
            h2 = norm_rows(row.astype(F32), wide(s2_ref), wide(b2_ref))
            xb[0, c, sub, :1024] = h2
            size = h2.shape[0]
            logit = lax.dot_general(wr_ref[...], h2, (((1,), (1,)), ((), ())), preferred_element_type=F32)
            eid = lax.broadcasted_iota(jnp.int32, (32, size), 0)
            picked = eid == ids_ref[0:1, span]
            for m in range(1, 8):
                picked = picked | (eid == ids_ref[m:m + 1, span])
            logit = jnp.where(picked, logit, -jnp.inf)
            ex = jnp.exp(logit - jnp.max(logit, axis=0, keepdims=True))
            prob = ex / jnp.sum(ex, axis=0, keepdims=True)
            full = jnp.concatenate([prob, jnp.zeros((96, size), F32)], axis=0)
            xb[0, c, sub, 1024:] = jnp.transpose(full).astype(BF)
            go(FAR, *at)
            go(NEAR, *at)

    def hand_on(c):
        for at in pieces(PASS, c):
            arrive(FAR, *at)
            go(PASS, *at)

    def ready(c):
        for at in pieces(NEAR, c):
            arrive(NEAR, *at)
            arrive(PASS, *at)

    def give_back(c):
        for at in pieces(BACK3, c):
            go(BACK3, *at)
        for at in pieces(BACK1, c):
            go(BACK1, *at)

    def far_sum(c):
        for at in pieces(BACKX, c):
            arrive(BACK3, *at)
            sub, _ = rows_of(*at)
            fb[c, sub, :] = (ob[2, c, sub, :].astype(F32) + rb[1, c, sub, :].astype(F32)).astype(BF)
            go(BACKX, *at)

    def all_sum(c):
        for at in pieces(BACKY, c):
            arrive(BACK1, *at)
            arrive(BACKX, *at)
            sub, _ = rows_of(*at)
            tb[c, sub, :] = (ob[0, c, sub, :].astype(F32) + rb[0, c, sub, :].astype(F32) + rf[c, sub, :].astype(F32)).astype(BF)
            go(BACKY, *at)

    def last_sum(c):
        for at in pieces(BACKY, c):
            arrive(BACKY, *at)
            sub, span = rows_of(*at)
            moe = tb[c, sub, :].astype(F32) + ry[c, sub, :].astype(F32)
            out_ref[span, :] = (x1[span, :].astype(F32) + moe).astype(BF)

    for c in range(n_c):
        for at in pieces(PART, c):
            go(PART, *at)
    mid(0)
    mid(1)
    hand_on(0)
    for one in loads:
        one.wait()
    table = {
        0: [(ready, 0)], 1: [(mid, 2)], 3: [(hand_on, 1)],
        4: [(give_back, 0), (ready, 1)], 5: [(mid, 3)], 6: [(far_sum, 0)], 7: [(hand_on, 2)],
        8: [(give_back, 1), (ready, 2)], 10: [(far_sum, 1)], 11: [(hand_on, 3)],
        12: [(give_back, 2), (ready, 3)], 13: [(all_sum, 0)], 14: [(far_sum, 2)],
    }
    parts = 4
    unit_row = lax.broadcasted_iota(jnp.int32, (128, 128 * n_e // parts), 0)
    unit_col = lax.broadcasted_iota(jnp.int32, (128, 128 * n_e // parts), 1) // 128

    def step(s, carry):
        for k, acts in table.items():
            @pl.when(s == k)
            def _():
                for act, c in acts:
                    act(c)
        c, q = s // parts, lax.rem(s, parts)

        @pl.when(q == 0)
        def _():
            acc[...] = jnp.zeros_like(acc)

        x = jnp.concatenate([xb[n, c, :, :1024] for n in range(4)], axis=0)
        gates = jnp.concatenate([xb[n, c, :, 1024:] for n in range(4)], axis=0)
        unit = (unit_row == me_ep * n_e + q * (n_e // parts) + unit_col).astype(F32).astype(BF)
        wide_gates = jnp.dot(gates, unit, preferred_element_type=F32)
        for m in range(n_e // parts):
            e = q * (n_e // parts) + m
            gate = jnp.dot(x, wg[e], preferred_element_type=F32)
            up = jnp.dot(x, wu[e], preferred_element_type=F32)
            act = (gate * jax.nn.sigmoid(gate) * up).astype(BF)
            y = jnp.dot(act, wd[e], preferred_element_type=F32)
            acc[...] += jnp.concatenate([wide_gates[:, m * 128:(m + 1) * 128]] * 8, axis=1) * y

        @pl.when(q == parts - 1)
        def _():
            for n in range(4):
                ob[n, c] = acc[n * rows:(n + 1) * rows, :].astype(BF)
        return carry

    lax.fori_loop(0, n_c * parts, step, 0)
    give_back(3)
    all_sum(1)
    far_sum(3)
    all_sum(2)
    last_sum(0)
    last_sum(1)
    all_sum(3)
    last_sum(2)
    last_sum(3)
    for kind in range(8):
        for c in range(n_c):
            for at in pieces(kind, c):
                move(kind, *at).wait_send()


def moe_layer(hidden, part, b_out, s2, b2, wr_t, ids, wg, wu, wd):
    n_batch = hidden.shape[0]
    rows = n_batch // CHUNKS
    vmem = pl.BlockSpec(memory_space=pltpu.VMEM)
    hbm = pl.BlockSpec(memory_space=pl.ANY)
    blocks = lambda *lead: pltpu.VMEM(lead + (CHUNKS, rows, 1024), BF)
    return pl.pallas_call(
        moe_kernel,
        in_specs=[vmem] * 7 + [hbm] * 3, out_specs=vmem,
        out_shape=jax.ShapeDtypeStruct((n_batch, 1024), BF),
        scratch_shapes=[
            pltpu.VMEM((n_batch, 1024), BF), pltpu.VMEM((n_batch, 1024), BF), pltpu.VMEM((4, CHUNKS, rows, WIDE), BF),
            pltpu.VMEM(wg.shape, BF), pltpu.VMEM(wu.shape, BF), pltpu.VMEM(wd.shape, BF),
            pltpu.VMEM((4 * rows, 1024), F32), blocks(4), blocks(2), blocks(), blocks(), blocks(), blocks(),
            pltpu.SemaphoreType.DMA((3,)), pltpu.SemaphoreType.DMA((8, 4 * CHUNKS)), pltpu.SemaphoreType.DMA((8, 4 * CHUNKS))],
        compiler_params=pltpu.CompilerParams(collective_id=0, has_side_effects=True, vmem_limit_bytes=VMEM_LIMIT),
        cost_estimate=pl.CostEstimate(flops=26_000_000_000, bytes_accessed=14_000_000, transcendentals=0),
        name="moe",
    )(part, hidden, b_out, s2, b2, wr_t, ids, wg, wu, wd)


def solution(mesh):
    token_rows = P(('dp', 'ep'), None)
    token_vec = P(('dp', 'ep'))
    cache_spec = P(('dp', 'ep'), None, 'tp', None)
    expert_in = P('ep', None, 'tp')
    expert_down = P('ep', 'tp', None)

    def device_step(hidden, seq_lens, rope_cos, rope_sin, ln1_scale, ln1_bias, w_qkv, b_qkv, w_out, b_out, k_cache, v_cache, ln2_scale, ln2_bias, w_router, expert_ids, w_gate, w_up, w_down):
        n_batch = hidden.shape[0]
        kt, vt = (jnp.transpose(c, (0, 2, 3, 1)) for c in (k_cache, v_cache))
        part, *caches = attention(0, n_batch, seq_lens, hidden, rope_cos.T, rope_sin.T, ln1_scale, ln1_bias, w_qkv, b_qkv, w_out, kt, vt, None)
        out = moe_layer(hidden, part, b_out, ln2_scale, ln2_bias, w_router.T, expert_ids.T, w_gate, w_up, w_down)
        return out, *(jnp.transpose(c, (0, 3, 1, 2)) for c in caches)

    in_specs = (token_rows, token_vec, token_rows, token_rows, P(), P(), P(None, 'tp'), P('tp'), P('tp', None), P(), cache_spec, cache_spec, P(), P(), P(), token_rows, expert_in, expert_in, expert_down)
    step = jax.shard_map(device_step, mesh=mesh, in_specs=in_specs, out_specs=(token_rows, cache_spec, cache_spec), check_vma=False)
    return step
```
